32 devices in a mesh: blk: 16 (over z, y, core), tile: 2 (over x).
Axes of the slice: x: 2, y: 2, z: 4, core: 2. Of those that a mesh axis runs over, the one named last changes fastest.
Arguments:
- positions: float32 [3, 2048], P(None, ('blk', 'tile')), as said below
- noise_vectors: float32 [3, 32, 2048], P(None, None, ('blk', 'tile')), may hold values from -6 to 6
- spectrum_bounds: float32 [2], replicated, as said below
Outputs:
- displacement: float32 [3, 32, 2048], P(None, None, ('blk', 'tile'))
- images: float32 [2, 3, 32, 2048], P(None, None, None, ('blk', 'tile'))
The draws below stay inside these ranges and needn't reach their ends.
Inputs may be any that keep to these rules, and one draw needn't show every extreme that they name: `positions`: coordinates lie in a cube whose edge is the cube root of 41.9 * 2048; particle n's third coordinate lies between n and n + 1 times that edge divided by 2048. `spectrum_bounds`: the first entry lies between 0.15 and 0.35; the second exceeds 50 times the first.
All inputs are finite; a program needn't handle non-finite values.
Results may differ from the reference program's by a relative error of at most 0.0003.
Values sent between devices are 32-bit elements; how exact they have to be, the bound alone decides.
No kernel may reach another device: no remote copies, remote signals or barrier semaphores. Data moves between devices by JAX's collectives and lax.ppermute only.
A program may use at most 64 MiB of HBM per device.

```python
import math
import jax
import jax.numpy as jnp
from jax import lax

PART_DEV = 64
NOISE = 32
NPART = 2048


def cube_edge():
    return (41.9 * NPART) ** (1.0 / 3.0)


def draw_positions(key, part):
    edge_value = cube_edge()
    split_keys = jax.random.split(key, 2)
    lateral = jax.random.uniform(split_keys[0], (2, NPART), jnp.float32)
    height_axis = (jnp.arange(NPART, dtype=jnp.float32) + jax.random.uniform(split_keys[1], (NPART,), jnp.float32)) * (edge_value / NPART)
    return jnp.concatenate([lateral * edge_value, height_axis[None, :]], axis=0)


def draw_noise_vectors(key, part):
    split_keys = jax.random.split(jax.random.fold_in(key, 17), 1)
    return jax.random.truncated_normal(split_keys[0], -6.0, 6.0, (3, NOISE, NPART), jnp.float32)


def draw_spectrum_bounds(key, part):
    estimate = 2.5 * NPART / cube_edge()
    sample = jax.random.uniform(key, (2,), jnp.float32)
    return jnp.stack([0.15 + 0.2 * sample[0], estimate * (0.9 + 0.4 * sample[1])])


def setup_inputs(seed: int = 0) -> dict:
    splits = jax.random.split(jax.random.key(seed), 4)
    positions = draw_positions(jax.random.fold_in(splits[3], 71), 0)
    noise_vectors = draw_noise_vectors(jax.random.fold_in(splits[3], 71), 0)
    spectrum_bounds = draw_spectrum_bounds(jax.random.fold_in(splits[3], 71), 0)
    return dict(positions=positions, noise_vectors=noise_vectors, spectrum_bounds=spectrum_bounds)


soft_core = 1e-06
node_count = 32

def kernel(targets, sources):
    offset = targets[:, :, None] - sources[:, None, :]
    squared = lax.optimization_barrier(jnp.sum(offset * offset, axis=0)) + soft_core
    distance = jnp.sqrt(squared)
    inverse = 1.0 / distance
    cubed = inverse * inverse * inverse
    intersection = distance < 2.0
    scalar_part = jnp.where(intersection, 1.0 - 0.28125 * distance, 0.75 * inverse + 0.5 * cubed)
    dyadic_part = jnp.where(intersection, 0.09375 * inverse, 0.75 * cubed - 1.5 * cubed * inverse * inverse)
    identity = jnp.eye(3, dtype=targets.dtype)
    return identity[:, :, None, None] * scalar_part[None, None] + dyadic_part[None, None] * offset[:, None] * offset[None, :]

def contract(tensor, vectors):
    return jnp.einsum('abij,bkj->aki', tensor, vectors, precision=lax.Precision.HIGHEST)

def weights_from(bounds):
    lowest = bounds[0]
    highest = bounds[1]
    center = 0.5 * (highest + lowest)
    spread = 0.5 * (highest - lowest)
    angles = math.pi * (jnp.arange(node_count, dtype=bounds.dtype) + 0.5) / node_count
    samples = jnp.sqrt(center + spread * jnp.cos(angles))
    weights = [2.0 / node_count * jnp.sum(samples * jnp.cos(order * angles)) for order in range(3)]
    return (center, spread, weights)

def mobility(vectors, positions):
    groups = NPART // PART_DEV
    targets = positions.reshape(3, groups, PART_DEV).transpose(1, 0, 2)

    def one_group(target_rows):
        return contract(kernel(target_rows, positions), vectors)
    pieces = lax.map(one_group, targets)
    return pieces.transpose(1, 2, 0, 3).reshape(3, vectors.shape[1], NPART)

def reference(positions, noise_vectors, spectrum_bounds):
    center, spread, weights = weights_from(spectrum_bounds)
    first_image = mobility(noise_vectors, positions)
    linear_term = (first_image - center * noise_vectors) / spread
    second_image = mobility(linear_term, positions)
    quadratic_term = 2.0 * (second_image - center * linear_term) / spread - noise_vectors
    displacement = 0.5 * weights[0] * noise_vectors + weights[1] * linear_term + weights[2] * quadratic_term
    return (displacement, jnp.stack([first_image, second_image]))
```

```python
import math

import jax
import jax.numpy as jnp
import numpy as np
from jax import lax
from jax.experimental import pallas as pl
from jax.experimental.pallas import tpu as pltpu
from jax.sharding import PartitionSpec as P

soft_core = 1e-06
node_count = 32
axes = ("blk", "tile")
pairs = ((0, 0), (0, 1), (0, 2), (1, 1), (1, 2), (2, 2))
f32 = jnp.float32
bf16 = jnp.bfloat16


def exchange(block, mask):
    count = lax.axis_size("blk") * lax.axis_size("tile")
    return lax.ppermute(block, axes, [(i, i ^ mask) for i in range(count)])


def pack_kernel(noise, positions, message):
    half = noise.shape[0] // 2
    message[0:half, :] = jnp.concatenate([noise[0:half, :], noise[half:, :]], axis=1)
    spot = positions[...]
    pad = jnp.zeros((8 - spot.shape[0], spot.shape[1]), f32)
    spot = jnp.concatenate([spot, pad], axis=0)
    message[half:, :] = jnp.concatenate([spot, spot], axis=1)


def halves(value):
    high = value.astype(bf16)
    return high, (value - high.astype(f32)).astype(bf16)


def unpack_pair(first, second, half):
    width = first.shape[1] // 2
    left = lax.broadcasted_iota(jnp.int32, (1, 2 * width), 1) < width
    first_rolled = pltpu.roll(first, width, 1)
    second_rolled = pltpu.roll(second, width, 1)
    upper = jnp.where(left, first, second_rolled)
    lower = jnp.where(left, first_rolled, second)
    return upper[:half], lower[:half], upper[half:]


def build_tiles(columns, target_rows, high, low):
    source_count = columns.shape[1]
    tile_count = target_rows.shape[1] // 128
    chunk = 16

    def one_chunk(step, carry):
        start = pl.multiple_of(step * chunk, chunk)
        source = [columns[c, pl.ds(start, chunk), :] for c in range(3)]
        for tile in range(tile_count):
            lanes = slice(tile * 128, (tile + 1) * 128)
            offset = [source[c] - target_rows[c : c + 1, lanes] for c in range(3)]
            squared = offset[0] * offset[0] + offset[1] * offset[1] + offset[2] * offset[2]
            squared = squared + soft_core
            inverse = lax.rsqrt(squared)
            distance = squared * inverse
            inverse_squared = inverse * inverse
            cubed = inverse * inverse_squared
            near = distance < 2.0
            scalar = jnp.where(near, 1.0 - 0.28125 * distance, 0.75 * inverse + 0.5 * cubed)
            dyadic = jnp.where(near, 0.09375 * inverse, cubed * (0.75 - 1.5 * inverse_squared))
            scaled = [dyadic * offset[c] for c in range(3)]
            for number, (a, b) in enumerate(pairs):
                value = scaled[a] * offset[b]
                if a == b:
                    value = value + scalar
                top, rest = halves(value)
                high[number, pl.ds(start, chunk), lanes] = top
                low[number, pl.ds(start, chunk), lanes] = rest
        return carry

    lax.fori_loop(0, source_count // chunk, one_chunk, 0)


def fill_columns(columns, rows):
    for c in range(3):
        for tile in range(rows.shape[1] // 128):
            lanes = slice(tile * 128, (tile + 1) * 128)
            wide = jnp.broadcast_to(rows[c : c + 1, lanes], (128, 128))
            columns[c, lanes, :] = wide.T


def apply_tiles(field, high, low):
    count = field[0].shape[0]
    parts = [halves(value) for value in field]
    both = [jnp.concatenate(part, axis=0) for part in parts]
    result = [None, None, None]

    def add(component, value):
        result[component] = value if result[component] is None else result[component] + value

    def dot(left, right):
        return jnp.dot(left, right, preferred_element_type=f32)

    for number, (a, b) in enumerate(pairs):
        if a == b:
            product = dot(both[a], high[number])
            add(a, product[:count] + product[count:])
            add(a, dot(parts[a][0], low[number]))
        else:
            product = dot(jnp.concatenate([both[a], both[b]], axis=0), high[number])
            add(b, product[:count] + product[count : 2 * count])
            add(a, product[2 * count : 3 * count] + product[3 * count :])
            product = dot(jnp.concatenate([parts[a][0], parts[b][0]], axis=0), low[number])
            add(b, product[:count])
            add(a, product[count:])
    return result


def first_kernel(bounds, blocks, near_positions, noise, partial, message, columns, rows, high, low):
    half = noise.shape[0] // 2
    vectors = noise.shape[0] // 3
    width = noise.shape[1]
    count = blocks.shape[0]
    uppers, lowers = [], []
    for number in range(0, count, 2):
        upper, lower, spots = unpack_pair(blocks[number], blocks[number + 1], half)
        uppers.append(upper)
        lowers.append(lower)
        rows[:, number * width : (number + 2) * width] = spots
    fill_columns(columns, rows)
    build_tiles(columns, near_positions, high, low)
    field = jnp.concatenate([jnp.concatenate(uppers, axis=1), jnp.concatenate(lowers, axis=1)], axis=0)
    field = [field[c * vectors : (c + 1) * vectors] for c in range(3)]
    value = jnp.concatenate(apply_tiles(field, high, low), axis=0)
    partial[...] = value
    message[...] = value
    center = 0.5 * (bounds[1] + bounds[0])
    message[:, :width] = value[:, :width] - center * noise[...]


def second_kernel(near_positions, blocks, bounds, nodes, high, low, weights, columns, rows):
    half = blocks.shape[1] - 8
    width = blocks.shape[2] // 2
    for number in range(0, blocks.shape[0], 2):
        spots = unpack_pair(blocks[number], blocks[number + 1], half)[2]
        rows[:, number * width : (number + 2) * width] = spots
    fill_columns(columns, near_positions)
    build_tiles(columns, rows, high, low)
    center = 0.5 * (bounds[1] + bounds[0])
    spread = 0.5 * (bounds[1] - bounds[0])
    samples = jnp.sqrt(jnp.where(nodes[3:4, :] > 0.0, center + spread * nodes[1:2, :], 0.0))
    total = jnp.sum(samples * nodes[...], axis=1, keepdims=True)
    weights[...] = jnp.broadcast_to((2.0 / node_count) * total, weights.shape)


def swapped(value, offset, width):
    count = value.shape[1] // width
    if offset == 0:
        return value
    tiles = [value[:, 128 * t : 128 * (t + 1)] for t in range(count * width // 128)]
    per_tile = 128 // width
    inner, outer = offset % per_tile, offset // per_tile
    tiles = [tiles[t ^ outer] for t in range(len(tiles))]
    if inner:
        tiles = [pltpu.roll(tile, width, 1) for tile in tiles]
    return tiles[0] if len(tiles) == 1 else jnp.concatenate(tiles, axis=1)


def third_kernel(bounds, *refs):
    received = refs[:-7]
    partial, message, high, low, first_image, kept, sent = refs[-7:]
    rows_count = partial.shape[0]
    width = first_image.shape[1]
    vectors = rows_count // 3
    spread = 0.5 * (bounds[1] - bounds[0])
    total = message[...]
    own = partial[:, :width]
    for number, ref in enumerate(received):
        part = swapped(ref[...], number + 1, width)
        total = total + part
        own = own + part[:, :width]
    first_image[...] = own
    linear = total / spread
    field = [linear[c * vectors : (c + 1) * vectors] for c in range(3)]
    value = jnp.concatenate(apply_tiles(field, high, low), axis=0)
    middle = value.shape[1] // 2
    kept[...] = value[:, :middle]
    sent[...] = value[:, middle:]


def fourth_kernel(kept, arrived, own, *outgoing):
    half = kept.shape[0] // 2
    width = own.shape[1] // 2
    total = kept[...] + arrived[...]
    for number, ref in enumerate((own, *outgoing)):
        block = total[:, number * width : (number + 1) * width]
        ref[...] = jnp.concatenate([block[:half], block[half:]], axis=1)


def final_kernel(bounds, weights, noise, first_image, own, *refs):
    received, (displacement, images) = refs[:-2], refs[-2:]
    width = noise.shape[1]
    total = own[...]
    for ref in received:
        total = total + ref[...]
    second = jnp.concatenate([total[:, :width], total[:, width:]], axis=0)
    center = 0.5 * (bounds[1] + bounds[0])
    spread = 0.5 * (bounds[1] - bounds[0])
    vectors = noise[...]
    first = first_image[...]
    linear = (first - center * vectors) / spread
    quadratic = 2.0 * (second - center * linear) / spread - vectors
    displacement[...] = (
        0.5 * weights[0:1, :width] * vectors
        + weights[1:2, :width] * linear
        + weights[2:3, :width] * quadratic
    )
    images[0] = first
    images[1] = second


smem = pl.BlockSpec(memory_space=pltpu.SMEM)
vmem = pl.BlockSpec(memory_space=pltpu.VMEM)


def call(kernel, inputs, in_specs, outputs, scratch=()):
    return pl.pallas_call(
        kernel,
        in_specs=in_specs,
        out_shape=[jax.ShapeDtypeStruct(shape, dtype) for shape, dtype in outputs],
        out_specs=[vmem] * len(outputs),
        scratch_shapes=list(scratch),
    )(*inputs)


def node_table():
    angles = math.pi * (np.arange(node_count) + 0.5) / node_count
    table = np.zeros((8, 128), np.float32)
    for order in range(3):
        table[order, :node_count] = np.cos(order * angles)
    table[3, :node_count] = 1.0
    return table


def combinations(masks):
    result = [0]
    for mask in masks:
        result += [value ^ mask for value in result]
    return result


def body(positions, noise_vectors, spectrum_bounds):
    tiles = lax.axis_size("tile")
    bits = lax.axis_size("blk").bit_length() - 1
    half_bits = bits // 2
    core_mask = tiles
    far_masks = [tiles << bit for bit in reversed(range(half_bits, bits))]
    near_masks = [1 << bit for bit in range(tiles.bit_length() - 1)]
    near_masks += [tiles << bit for bit in range(1, half_bits)]
    components, vectors, width = noise_vectors.shape
    rows = components * vectors
    noise = noise_vectors.reshape(rows, width)
    bounds = spectrum_bounds

    (packed,) = call(
        pack_kernel, (noise, positions), [vmem, vmem], [((rows // 2 + 8, 2 * width), f32)]
    )
    far = packed[None]
    near = positions
    for mask in far_masks:
        far = jnp.concatenate([far, exchange(far, mask)], axis=0)
    for mask in near_masks:
        near = jnp.concatenate([near, exchange(near, mask)], axis=1)
    blocks = jnp.concatenate([far, exchange(far, core_mask)], axis=0)
    near_count, far_count = near.shape[1], blocks.shape[0] * width

    partial, message = call(
        first_kernel,
        (bounds, blocks, near, noise),
        [smem, vmem, vmem, vmem],
        [((rows, near_count), f32)] * 2,
        (
            pltpu.VMEM((3, far_count, 128), f32),
            pltpu.VMEM((8, far_count), f32),
            pltpu.VMEM((6, far_count, near_count), bf16),
            pltpu.VMEM((6, far_count, near_count), bf16),
        ),
    )
    high, low, weights = call(
        second_kernel,
        (near, blocks, bounds, jnp.asarray(node_table())),
        [vmem, vmem, smem, vmem],
        [((6, near_count, far_count), bf16)] * 2 + [((8, 128), f32)],
        (pltpu.VMEM((3, near_count, 128), f32), pltpu.VMEM((8, far_count), f32)),
    )
    received = [exchange(message, mask) for mask in combinations(near_masks)[1:]]
    first_image, kept, sent = call(
        third_kernel,
        (bounds, *received, partial, message, high, low),
        [smem] + [vmem] * (len(received) + 4),
        [((rows, width), f32), ((rows, far_count // 2), f32), ((rows, far_count // 2), f32)],
    )
    arrived = exchange(sent, core_mask)
    far_steps = combinations(far_masks)
    own, *outgoing = call(
        fourth_kernel,
        (kept, arrived),
        [vmem, vmem],
        [((rows // 2, 2 * width), f32)] * len(far_steps),
    )
    received = [exchange(block, mask) for block, mask in zip(outgoing, far_steps[1:])]
    displacement, images = call(
        final_kernel,
        (bounds, weights, noise, first_image, own, *received),
        [smem] + [vmem] * (4 + len(received)),
        [((rows, width), f32), ((2, rows, width), f32)],
    )
    shape = noise_vectors.shape
    return displacement.reshape(shape), images.reshape((2, *shape))


def solution(mesh):
    return jax.shard_map(
        body,
        mesh=mesh,
        in_specs=(P(None, axes), P(None, None, axes), P()),
        out_specs=(P(None, None, axes), P(None, None, None, axes)),
        check_vma=False,
    )
```

```python
import math

import jax
import jax.numpy as jnp
import numpy as np
from jax import lax
from jax.experimental import pallas as pl
from jax.experimental.pallas import tpu as pltpu
from jax.sharding import PartitionSpec as P

soft_core = 1e-06
node_count = 32
spare_bytes = 8 << 20
axes = ("blk", "tile")
pairs = ((0, 0), (0, 1), (0, 2), (1, 1), (1, 2), (2, 2))
f32 = jnp.float32
bf16 = jnp.bfloat16


def exchange(block, mask):
    count = lax.axis_size("blk") * lax.axis_size("tile")
    return lax.ppermute(block, axes, [(i, i ^ mask) for i in range(count)])


def pack_kernel(noise, positions, message):
    half = noise.shape[0] // 2
    message[0:half, :] = jnp.concatenate([noise[0:half, :], noise[half:, :]], axis=1)
    spot = positions[...]
    pad = jnp.zeros((8 - spot.shape[0], spot.shape[1]), f32)
    spot = jnp.concatenate([spot, pad], axis=0)
    message[half:, :] = jnp.concatenate([spot, spot], axis=1)


def halves(value):
    high = value.astype(bf16)
    return high, (value - high.astype(f32)).astype(bf16)


def unpack_pair(first, second, half):
    width = first.shape[1] // 2
    left = lax.broadcasted_iota(jnp.int32, (1, 2 * width), 1) < width
    first_rolled = pltpu.roll(first, width, 1)
    second_rolled = pltpu.roll(second, width, 1)
    upper = jnp.where(left, first, second_rolled)
    lower = jnp.where(left, first_rolled, second)
    return upper[:half], lower[:half], upper[half:]


def build_tiles(columns, target_rows, high, low):
    source_count = columns.shape[1]
    tile_count = target_rows.shape[1] // 128
    chunk = 16

    def one_chunk(step, carry):
        start = pl.multiple_of(step * chunk, chunk)
        source = [columns[c, pl.ds(start, chunk), :] for c in range(3)]
        for tile in range(tile_count):
            lanes = slice(tile * 128, (tile + 1) * 128)
            offset = [source[c] - target_rows[c : c + 1, lanes] for c in range(3)]
            squared = offset[0] * offset[0] + offset[1] * offset[1] + offset[2] * offset[2]
            squared = squared + soft_core
            inverse = lax.rsqrt(squared)
            distance = squared * inverse
            inverse_squared = inverse * inverse
            cubed = inverse * inverse_squared
            near = distance < 2.0
            scalar = jnp.where(near, 1.0 - 0.28125 * distance, 0.75 * inverse + 0.5 * cubed)
            dyadic = jnp.where(near, 0.09375 * inverse, cubed * (0.75 - 1.5 * inverse_squared))
            scaled = [dyadic * offset[c] for c in range(3)]
            for number, (a, b) in enumerate(pairs):
                value = scaled[a] * offset[b]
                if a == b:
                    value = value + scalar
                top, rest = halves(value)
                high[number, pl.ds(start, chunk), lanes] = top
                low[number, pl.ds(start, chunk), lanes] = rest
        return carry

    lax.fori_loop(0, source_count // chunk, one_chunk, 0)


def fill_columns(columns, rows):
    for c in range(3):
        for tile in range(rows.shape[1] // 128):
            lanes = slice(tile * 128, (tile + 1) * 128)
            wide = jnp.broadcast_to(rows[c : c + 1, lanes], (128, 128))
            columns[c, lanes, :] = wide.T


def apply_tiles(field, high, low):
    count = field[0].shape[0]
    parts = [halves(value) for value in field]
    both = [jnp.concatenate(part, axis=0) for part in parts]
    result = [None, None, None]

    def add(component, value):
        result[component] = value if result[component] is None else result[component] + value

    def dot(left, right):
        return jnp.dot(left, right, preferred_element_type=f32)

    for number, (a, b) in enumerate(pairs):
        if a == b:
            product = dot(both[a], high[number])
            add(a, product[:count] + product[count:])
            add(a, dot(parts[a][0], low[number]))
        else:
            product = dot(jnp.concatenate([both[a], both[b]], axis=0), high[number])
            add(b, product[:count] + product[count : 2 * count])
            add(a, product[2 * count : 3 * count] + product[3 * count :])
            product = dot(jnp.concatenate([parts[a][0], parts[b][0]], axis=0), low[number])
            add(b, product[:count])
            add(a, product[count:])
    return result


def first_kernel(bounds, blocks, near_positions, noise, partial, message, columns, rows, high, low):
    half = noise.shape[0] // 2
    vectors = noise.shape[0] // 3
    width = noise.shape[1]
    count = blocks.shape[0]
    uppers, lowers = [], []
    for number in range(0, count, 2):
        upper, lower, spots = unpack_pair(blocks[number], blocks[number + 1], half)
        uppers.append(upper)
        lowers.append(lower)
        rows[:, number * width : (number + 2) * width] = spots
    fill_columns(columns, rows)
    build_tiles(columns, near_positions, high, low)
    field = jnp.concatenate([jnp.concatenate(uppers, axis=1), jnp.concatenate(lowers, axis=1)], axis=0)
    field = [field[c * vectors : (c + 1) * vectors] for c in range(3)]
    value = jnp.concatenate(apply_tiles(field, high, low), axis=0)
    partial[...] = value
    message[...] = value
    center = 0.5 * (bounds[1] + bounds[0])
    message[:, :width] = value[:, :width] - center * noise[...]


def second_kernel(bounds, near_positions, blocks, nodes, high, low, weights, columns, rows):
    half = blocks.shape[1] - 8
    width = blocks.shape[2] // 2
    for number in range(0, blocks.shape[0], 2):
        spots = unpack_pair(blocks[number], blocks[number + 1], half)[2]
        rows[:, number * width : (number + 2) * width] = spots
    fill_columns(columns, near_positions)
    build_tiles(columns, rows, high, low)
    center = 0.5 * (bounds[1] + bounds[0])
    spread = 0.5 * (bounds[1] - bounds[0])
    samples = jnp.sqrt(jnp.where(nodes[3:4, :] > 0.0, center + spread * nodes[1:2, :], 0.0))
    total = jnp.sum(samples * nodes[...], axis=1, keepdims=True)
    weights[...] = jnp.broadcast_to((2.0 / node_count) * total, weights.shape)


def swapped(value, offset, width):
    count = value.shape[1] // width
    if offset == 0:
        return value
    tiles = [value[:, 128 * t : 128 * (t + 1)] for t in range(count * width // 128)]
    per_tile = 128 // width
    inner, outer = offset % per_tile, offset // per_tile
    tiles = [tiles[t ^ outer] for t in range(len(tiles))]
    if inner:
        tiles = [pltpu.roll(tile, width, 1) for tile in tiles]
    return tiles[0] if len(tiles) == 1 else jnp.concatenate(tiles, axis=1)


def third_kernel(bounds, *refs):
    received = refs[:-7]
    partial, message, high, low, first_image, kept, sent = refs[-7:]
    rows_count = partial.shape[0]
    width = first_image.shape[1]
    vectors = rows_count // 3
    spread = 0.5 * (bounds[1] - bounds[0])
    total = message[...]
    own = partial[:, :width]
    for number, ref in enumerate(received):
        part = swapped(ref[...], number + 1, width)
        total = total + part
        own = own + part[:, :width]
    first_image[...] = own
    linear = total / spread
    field = [linear[c * vectors : (c + 1) * vectors] for c in range(3)]
    value = jnp.concatenate(apply_tiles(field, high, low), axis=0)
    middle = value.shape[1] // 2
    kept[...] = value[:, :middle]
    sent[...] = value[:, middle:]


def fourth_kernel(kept, arrived, own, *outgoing):
    half = kept.shape[0] // 2
    width = own.shape[1] // 2
    total = kept[...] + arrived[...]
    for number, ref in enumerate((own, *outgoing)):
        block = total[:, number * width : (number + 1) * width]
        ref[...] = jnp.concatenate([block[:half], block[half:]], axis=1)


def final_kernel(bounds, weights, noise, first_image, own, *refs):
    received, (displacement, images) = refs[:-2], refs[-2:]
    width = noise.shape[1]
    total = own[...]
    for ref in received:
        total = total + ref[...]
    second = jnp.concatenate([total[:, :width], total[:, width:]], axis=0)
    center = 0.5 * (bounds[1] + bounds[0])
    spread = 0.5 * (bounds[1] - bounds[0])
    vectors = noise[...]
    first = first_image[...]
    linear = (first - center * vectors) / spread
    quadratic = 2.0 * (second - center * linear) / spread - vectors
    displacement[...] = (
        0.5 * weights[0:1, :width] * vectors
        + weights[1:2, :width] * linear
        + weights[2:3, :width] * quadratic
    )
    images[0] = first
    images[1] = second


smem = pl.BlockSpec(memory_space=pltpu.SMEM)
vmem = pl.BlockSpec(memory_space=pltpu.VMEM)


def call(kernel, inputs, outputs, scratch=(), final=False):
    specs, arrays = [], []
    for value, place in inputs:
        specs.append(smem if place == "smem" else vmem)
        arrays.append(pltpu.with_memory_space_constraint(value, pltpu.VMEM) if place == "vmem" else value)
    make = jax.ShapeDtypeStruct if final else pltpu.VMEM
    sizes = [math.prod(ref.shape) * np.dtype(ref.dtype).itemsize for ref in scratch]
    return pl.pallas_call(
        kernel,
        in_specs=specs,
        out_shape=[make(shape, dtype) for shape, dtype in outputs],
        out_specs=[vmem] * len(outputs),
        scratch_shapes=list(scratch),
        compiler_params=pltpu.CompilerParams(vmem_limit_bytes=sum(sizes) + spare_bytes),
    )(*arrays)


def held(*values):
    return [(value, "vmem") for value in values]


def given(*values):
    return [(value, "") for value in values]


def node_table():
    angles = math.pi * (np.arange(node_count) + 0.5) / node_count
    table = np.zeros((8, 128), np.float32)
    for order in range(3):
        table[order, :node_count] = np.cos(order * angles)
    table[3, :node_count] = 1.0
    return table


def combinations(masks):
    result = [0]
    for mask in masks:
        result += [value ^ mask for value in result]
    return result


def body(positions, noise_vectors, spectrum_bounds):
    tiles = lax.axis_size("tile")
    bits = lax.axis_size("blk").bit_length() - 1
    half_bits = bits // 2
    core_mask = tiles
    far_masks = [tiles << bit for bit in reversed(range(half_bits, bits))]
    near_masks = [1 << bit for bit in range(tiles.bit_length() - 1)]
    near_masks += [tiles << bit for bit in range(1, half_bits)]
    components, vectors, width = noise_vectors.shape
    rows = components * vectors
    noise = noise_vectors.reshape(rows, width)
    bounds = spectrum_bounds

    (packed,) = call(pack_kernel, given(noise, positions), [((rows // 2 + 8, 2 * width), f32)])
    far = packed[None]
    near = positions
    for mask in far_masks:
        far = jnp.concatenate([far, exchange(far, mask)], axis=0)
    for mask in near_masks:
        near = jnp.concatenate([near, exchange(near, mask)], axis=1)
    blocks = jnp.concatenate([far, exchange(far, core_mask)], axis=0)
    near_count, far_count = near.shape[1], blocks.shape[0] * width
    scalars = [(bounds, "smem")]

    partial, message = call(
        first_kernel,
        scalars + held(blocks, near) + given(noise),
        [((rows, near_count), f32)] * 2,
        (
            pltpu.VMEM((3, far_count, 128), f32),
            pltpu.VMEM((8, far_count), f32),
            pltpu.VMEM((6, far_count, near_count), bf16),
            pltpu.VMEM((6, far_count, near_count), bf16),
        ),
    )
    high, low, weights = call(
        second_kernel,
        scalars + held(near, blocks) + given(jnp.asarray(node_table())),
        [((6, near_count, far_count), bf16)] * 2 + [((8, 128), f32)],
        (pltpu.VMEM((3, near_count, 128), f32), pltpu.VMEM((8, far_count), f32)),
    )
    received = [exchange(message, mask) for mask in combinations(near_masks)[1:]]
    first_image, kept, sent = call(
        third_kernel,
        scalars + held(*received, partial, message, high, low),
        [((rows, width), f32), ((rows, far_count // 2), f32), ((rows, far_count // 2), f32)],
    )
    arrived = exchange(sent, core_mask)
    far_steps = combinations(far_masks)
    own, *outgoing = call(
        fourth_kernel, held(kept, arrived), [((rows // 2, 2 * width), f32)] * len(far_steps)
    )
    received = [exchange(block, mask) for block, mask in zip(outgoing, far_steps[1:])]
    displacement, images = call(
        final_kernel,
        scalars + held(weights) + given(noise) + held(first_image, own, *received),
        [((rows, width), f32), ((2, rows, width), f32)],
        final=True,
    )
    shape = noise_vectors.shape
    return displacement.reshape(shape), images.reshape((2, *shape))


def solution(mesh):
    return jax.shard_map(
        body,
        mesh=mesh,
        in_specs=(P(None, axes), P(None, None, axes), P()),
        out_specs=(P(None, None, axes), P(None, None, None, axes)),
        check_vma=False,
    )
```

```python
import math

import jax
import jax.numpy as jnp
import numpy as np
from jax import lax
from jax.experimental import pallas as pl
from jax.experimental.pallas import tpu as pltpu
from jax.sharding import PartitionSpec as P

soft_core = 1e-06
node_count = 32
spare_bytes = 8 << 20
axes = ("blk", "tile")
pairs = ((0, 0), (0, 1), (0, 2), (1, 1), (1, 2), (2, 2))
f32 = jnp.float32
bf16 = jnp.bfloat16


def exchange(block, mask):
    count = lax.axis_size("blk") * lax.axis_size("tile")
    return lax.ppermute(block, axes, [(i, i ^ mask) for i in range(count)])


def open_kernel(
    noise_in, positions_in, bounds_in, nodes_in, message, noise, positions, scalars, nodes, bounds, sems
):
    moves = (
        (noise_in, noise),
        (positions_in, positions),
        (bounds_in, bounds),
        (nodes_in, nodes),
    )
    copies = [pltpu.make_async_copy(*move, sems.at[n]) for n, move in enumerate(moves)]
    for copy in copies:
        copy.start()
    for copy in copies:
        copy.wait()
    half = noise.shape[0] // 2
    message[0:half, :] = jnp.concatenate([noise[0:half, :], noise[half:, :]], axis=1)
    spot = positions[...]
    pad = jnp.zeros((8 - spot.shape[0], spot.shape[1]), f32)
    spot = jnp.concatenate([spot, pad], axis=0)
    message[half:, :] = jnp.concatenate([spot, spot], axis=1)
    highest, lowest = bounds[1], bounds[0]
    scalars[0:4, :] = jnp.full((4, 128), 0.5 * (highest + lowest), f32)
    scalars[4:8, :] = jnp.full((4, 128), 0.5 * (highest - lowest), f32)


def halves(value):
    high = value.astype(bf16)
    return high, (value - high.astype(f32)).astype(bf16)


def unpack_pair(first, second, half):
    width = first.shape[1] // 2
    left = lax.broadcasted_iota(jnp.int32, (1, 2 * width), 1) < width
    first_rolled = pltpu.roll(first, width, 1)
    second_rolled = pltpu.roll(second, width, 1)
    upper = jnp.where(left, first, second_rolled)
    lower = jnp.where(left, first_rolled, second)
    return upper[:half], lower[:half], upper[half:]


def build_tiles(columns, target_rows, high, low):
    source_count = columns.shape[1]
    tile_count = target_rows.shape[1] // 128
    chunk = 16

    def one_chunk(step, carry):
        start = pl.multiple_of(step * chunk, chunk)
        source = [columns[c, pl.ds(start, chunk), :] for c in range(3)]
        for tile in range(tile_count):
            lanes = slice(tile * 128, (tile + 1) * 128)
            offset = [source[c] - target_rows[c : c + 1, lanes] for c in range(3)]
            squared = offset[0] * offset[0] + offset[1] * offset[1] + offset[2] * offset[2]
            squared = squared + soft_core
            inverse = lax.rsqrt(squared)
            distance = squared * inverse
            inverse_squared = inverse * inverse
            cubed = inverse * inverse_squared
            near = distance < 2.0
            scalar = jnp.where(near, 1.0 - 0.28125 * distance, 0.75 * inverse + 0.5 * cubed)
            dyadic = jnp.where(near, 0.09375 * inverse, cubed * (0.75 - 1.5 * inverse_squared))
            scaled = [dyadic * offset[c] for c in range(3)]
            for number, (a, b) in enumerate(pairs):
                value = scaled[a] * offset[b]
                if a == b:
                    value = value + scalar
                top, rest = halves(value)
                high[number, pl.ds(start, chunk), lanes] = top
                low[number, pl.ds(start, chunk), lanes] = rest
        return carry

    lax.fori_loop(0, source_count // chunk, one_chunk, 0)


def fill_columns(columns, rows):
    for c in range(3):
        for tile in range(rows.shape[1] // 128):
            lanes = slice(tile * 128, (tile + 1) * 128)
            wide = jnp.broadcast_to(rows[c : c + 1, lanes], (128, 128))
            columns[c, lanes, :] = wide.T


def apply_tiles(field, high, low):
    count = field[0].shape[0]
    parts = [halves(value) for value in field]
    both = [jnp.concatenate(part, axis=0) for part in parts]
    result = [None, None, None]

    def add(component, value):
        result[component] = value if result[component] is None else result[component] + value

    def dot(left, right):
        return jnp.dot(left, right, preferred_element_type=f32)

    for number, (a, b) in enumerate(pairs):
        if a == b:
            product = dot(both[a], high[number])
            add(a, product[:count] + product[count:])
            add(a, dot(parts[a][0], low[number]))
        else:
            product = dot(jnp.concatenate([both[a], both[b]], axis=0), high[number])
            add(b, product[:count] + product[count : 2 * count])
            add(a, product[2 * count : 3 * count] + product[3 * count :])
            product = dot(jnp.concatenate([parts[a][0], parts[b][0]], axis=0), low[number])
            add(b, product[:count])
            add(a, product[count:])
    return result


def gather_rows(pieces, rows, half):
    uppers, lowers = [], []
    start = 0
    for piece in pieces:
        for number in range(0, piece.shape[0], 2):
            upper, lower, spots = unpack_pair(piece[number], piece[number + 1], half)
            uppers.append(upper)
            lowers.append(lower)
            rows[:, start : start + spots.shape[1]] = spots
            start += spots.shape[1]
    return uppers, lowers


def side_by_side(values):
    return values[0] if len(values) == 1 else jnp.concatenate(values, axis=1)


def product_of(pieces, near_positions, scratch):
    columns, rows, high, low = scratch
    half = pieces[0].shape[1] - 8
    vectors = 2 * half // 3
    uppers, lowers = gather_rows(pieces, rows, half)
    fill_columns(columns, rows)
    build_tiles(columns, near_positions, high, low)
    field = jnp.concatenate([side_by_side(uppers), side_by_side(lowers)], axis=0)
    field = [field[c * vectors : (c + 1) * vectors] for c in range(3)]
    return jnp.concatenate(apply_tiles(field, high, low), axis=0)


def opening_part(near_positions, *refs):
    pieces, total, scratch = refs[:-5], refs[-5], refs[-4:]
    total[...] = product_of(pieces, near_positions, scratch)


def middle_part(near_positions, before, *refs):
    pieces, total, scratch = refs[:-5], refs[-5], refs[-4:]
    total[...] = before[...] + product_of(pieces, near_positions, scratch)


def closing_part(scalars, noise, near_positions, before, *refs):
    pieces, (partial, message), scratch = refs[:-6], refs[-6:-4], refs[-4:]
    width = noise.shape[1]
    value = before[...] + product_of(pieces, near_positions, scratch)
    partial[...] = value
    message[...] = value
    message[:, :width] = value[:, :width] - scalars[0:1, :width] * noise[...]


def second_kernel(scalars, nodes, near_positions, *refs):
    pieces, (high, low, weights, columns, rows) = refs[:-5], refs[-5:]
    gather_rows(pieces, rows, pieces[0].shape[1] - 8)
    fill_columns(columns, near_positions)
    build_tiles(columns, rows, high, low)
    samples = scalars[0:1, :] + scalars[4:5, :] * nodes[1:2, :]
    samples = jnp.sqrt(jnp.where(nodes[3:4, :] > 0.0, samples, 0.0))
    total = jnp.sum(samples * nodes[...], axis=1, keepdims=True)
    weights[...] = jnp.broadcast_to((2.0 / node_count) * total, weights.shape)


def swapped(value, offset, width):
    count = value.shape[1] // width
    if offset == 0:
        return value
    tiles = [value[:, 128 * t : 128 * (t + 1)] for t in range(count * width // 128)]
    per_tile = 128 // width
    inner, outer = offset % per_tile, offset // per_tile
    tiles = [tiles[t ^ outer] for t in range(len(tiles))]
    if inner:
        tiles = [pltpu.roll(tile, width, 1) for tile in tiles]
    return tiles[0] if len(tiles) == 1 else jnp.concatenate(tiles, axis=1)


def third_kernel(scalars, *refs):
    received = refs[:-7]
    partial, message, high, low, first_image, linear, sent = refs[-7:]
    width = first_image.shape[1]
    total = message[...]
    own = partial[:, :width]
    for number, ref in enumerate(received):
        part = swapped(ref[...], number + 1, width)
        total = total + part
        own = own + part[:, :width]
    first_image[...] = own
    linear[...] = total / scalars[4:5, 0:1]
    half_product(linear, high, low, sent, 1)


def half_product(linear, high, low, out, side):
    vectors = linear.shape[0] // 3
    middle = high.shape[2] // 2
    lanes = slice(side * middle, (side + 1) * middle)
    field = [linear[c * vectors : (c + 1) * vectors, :] for c in range(3)]
    value = apply_tiles(field, high.at[:, :, lanes], low.at[:, :, lanes])
    out[...] = jnp.concatenate(value, axis=0)


def kept_kernel(linear, high, low, kept):
    half_product(linear, high, low, kept, 0)


def fourth_kernel(kept, arrived, own, *outgoing):
    half = kept.shape[0] // 2
    width = own.shape[1] // 2
    total = kept[...] + arrived[...]
    for number, ref in enumerate((own, *outgoing)):
        block = total[:, number * width : (number + 1) * width]
        ref[...] = jnp.concatenate([block[:half], block[half:]], axis=1)


def final_kernel(scalars, weights, noise, first_image, own, *refs):
    received, (displacement, images) = refs[:-2], refs[-2:]
    width = noise.shape[1]
    total = own[...]
    for ref in received:
        total = total + ref[...]
    second = jnp.concatenate([total[:, :width], total[:, width:]], axis=0)
    center = scalars[0:1, :width]
    spread = scalars[4:5, :width]
    vectors = noise[...]
    first = first_image[...]
    linear = (first - center * vectors) / spread
    quadratic = 2.0 * (second - center * linear) / spread - vectors
    displacement[...] = (
        0.5 * weights[0:1, :width] * vectors
        + weights[1:2, :width] * linear
        + weights[2:3, :width] * quadratic
    )
    images[0] = first
    images[1] = second


vmem = pl.BlockSpec(memory_space=pltpu.VMEM)


def call(kernel, inputs, outputs, scratch=(), final=False, opening=False):
    space = pltpu.HBM if opening else pltpu.VMEM
    make = jax.ShapeDtypeStruct if final else pltpu.VMEM
    sizes = [
        math.prod(ref.shape) * np.dtype(ref.dtype).itemsize
        for ref in scratch
        if ref.memory_space == pltpu.VMEM
    ]
    return pl.pallas_call(
        kernel,
        in_specs=[pl.BlockSpec(memory_space=space)] * len(inputs),
        out_shape=[make(shape, dtype) for shape, dtype in outputs],
        out_specs=[vmem] * len(outputs),
        scratch_shapes=list(scratch),
        compiler_params=pltpu.CompilerParams(vmem_limit_bytes=sum(sizes) + spare_bytes),
    )(*[pltpu.with_memory_space_constraint(value, space) for value in inputs])


def node_table():
    angles = math.pi * (np.arange(node_count) + 0.5) / node_count
    table = np.zeros((8, 128), np.float32)
    for order in range(3):
        table[order, :node_count] = np.cos(order * angles)
    table[3, :node_count] = 1.0
    return table


def combinations(masks):
    result = [0]
    for mask in masks:
        result += [value ^ mask for value in result]
    return result


def body(positions_in, noise_vectors, spectrum_bounds):
    tiles = lax.axis_size("tile")
    bits = lax.axis_size("blk").bit_length() - 1
    half_bits = bits // 2
    core_mask = tiles
    far_masks = [tiles << bit for bit in reversed(range(half_bits, bits))]
    near_masks = [1 << bit for bit in range(tiles.bit_length() - 1)]
    near_masks += [tiles << bit for bit in range(1, half_bits)]
    components, vectors, width = noise_vectors.shape
    rows = components * vectors
    last = len(far_masks) - 1
    block = ((rows // 2, 2 * width), f32)

    message, noise, positions, scalars, nodes = call(
        open_kernel,
        (
            noise_vectors.reshape(rows, width),
            positions_in,
            spectrum_bounds,
            jnp.asarray(node_table()),
        ),
        [
            ((rows // 2 + 8, 2 * width), f32),
            ((rows, width), f32),
            (positions_in.shape, f32),
            ((8, 128), f32),
            ((8, 128), f32),
        ],
        (pltpu.SMEM((2,), f32), pltpu.SemaphoreType.DMA((4,))),
        opening=True,
    )
    near = positions
    far = message[None]
    for mask in near_masks:
        near = jnp.concatenate([near, exchange(near, mask)], axis=1)
    for mask in far_masks[:last]:
        far = jnp.concatenate([far, exchange(far, mask)], axis=0)
    across = exchange(far, core_mask)
    late = exchange(far, far_masks[last])
    late_across = exchange(late, core_mask)
    near_count, piece_count = near.shape[1], far.shape[0] * width
    far_count = 4 * piece_count

    def tiles_for(count):
        return (
            pltpu.VMEM((3, count, 128), f32),
            pltpu.VMEM((8, count), f32),
            pltpu.VMEM((6, count, near_count), bf16),
            pltpu.VMEM((6, count, near_count), bf16),
        )

    whole = ((rows, near_count), f32)
    (total,) = call(opening_part, (near, far, across), [whole], tiles_for(2 * piece_count))
    (total,) = call(middle_part, (near, total, late), [whole], tiles_for(piece_count))
    partial, message = call(
        closing_part,
        (scalars, noise, near, total, late_across),
        [whole, whole],
        tiles_for(piece_count),
    )
    high, low, weights = call(
        second_kernel,
        (scalars, nodes, near, far, late, across, late_across),
        [((6, near_count, far_count), bf16)] * 2 + [((8, 128), f32)],
        (pltpu.VMEM((3, near_count, 128), f32), pltpu.VMEM((8, far_count), f32)),
    )
    near_steps = combinations(near_masks)
    received = [exchange(message, mask) for mask in near_steps[1:]]
    first_image, linear, sent = call(
        third_kernel,
        (scalars, *received, partial, message, high, low),
        [((rows, width), f32), whole, ((rows, far_count // 2), f32)],
    )
    arrived = exchange(sent, core_mask)
    (kept,) = call(kept_kernel, (linear, high, low), [((rows, far_count // 2), f32)])
    far_steps = combinations(far_masks)
    own, *outgoing = call(fourth_kernel, (kept, arrived), [block] * len(far_steps))
    received = [exchange(value, mask) for value, mask in zip(outgoing, far_steps[1:])]
    displacement, images = call(
        final_kernel,
        (scalars, weights, noise, first_image, own, *received),
        [((rows, width), f32), ((2, rows, width), f32)],
        final=True,
    )
    shape = noise_vectors.shape
    return displacement.reshape(shape), images.reshape((2, *shape))


def solution(mesh):
    return jax.shard_map(
        body,
        mesh=mesh,
        in_specs=(P(None, axes), P(None, None, axes), P()),
        out_specs=(P(None, None, axes), P(None, None, None, axes)),
        check_vma=False,
    )
```

```python
import math

import jax
import jax.numpy as jnp
import numpy as np
from jax import lax
from jax.experimental import pallas as pl
from jax.experimental.pallas import tpu as pltpu
from jax.sharding import PartitionSpec as P

soft_core = 1e-06
node_count = 32
spare_bytes = 8 << 20
axes = ("blk", "tile")
pairs = ((0, 0), (0, 1), (0, 2), (1, 1), (1, 2), (2, 2))
f32 = jnp.float32
bf16 = jnp.bfloat16


def exchange(block, mask):
    count = lax.axis_size("blk") * lax.axis_size("tile")
    return lax.ppermute(block, axes, [(i, i ^ mask) for i in range(count)])


def open_kernel(
    noise_in, positions_in, bounds_in, nodes_in, message, noise, positions, scalars, nodes, bounds, sems
):
    moves = (
        (noise_in, noise),
        (positions_in, positions),
        (bounds_in, bounds),
        (nodes_in, nodes),
    )
    copies = [pltpu.make_async_copy(*move, sems.at[n]) for n, move in enumerate(moves)]
    for copy in copies:
        copy.start()
    for copy in copies:
        copy.wait()
    half = noise.shape[0] // 2
    message[0:half, :] = jnp.concatenate([noise[0:half, :], noise[half:, :]], axis=1)
    spot = positions[...]
    pad = jnp.zeros((8 - spot.shape[0], spot.shape[1]), f32)
    spot = jnp.concatenate([spot, pad], axis=0)
    message[half:, :] = jnp.concatenate([spot, spot], axis=1)
    highest, lowest = bounds[1], bounds[0]
    scalars[0:4, :] = jnp.full((4, 128), 0.5 * (highest + lowest), f32)
    scalars[4:8, :] = jnp.full((4, 128), 0.5 * (highest - lowest), f32)


def halves(value):
    high = value.astype(bf16)
    return high, (value - high.astype(f32)).astype(bf16)


def unpack_pair(first, second, half):
    width = first.shape[1] // 2
    left = lax.broadcasted_iota(jnp.int32, (1, 2 * width), 1) < width
    first_rolled = pltpu.roll(first, width, 1)
    second_rolled = pltpu.roll(second, width, 1)
    upper = jnp.where(left, first, second_rolled)
    lower = jnp.where(left, first_rolled, second)
    return upper[:half], lower[:half], upper[half:]


def build_tiles(columns, target_rows, high, low):
    source_count = columns.shape[1]
    tile_count = target_rows.shape[1] // 128
    chunk = 32

    def one_chunk(step, carry):
        start = pl.multiple_of(step * chunk, chunk)
        source = [columns[c, pl.ds(start, chunk), :] for c in range(3)]
        for tile in range(tile_count):
            lanes = slice(tile * 128, (tile + 1) * 128)
            offset = [source[c] - target_rows[c : c + 1, lanes] for c in range(3)]
            squared = offset[0] * offset[0] + offset[1] * offset[1] + offset[2] * offset[2]
            squared = squared + soft_core
            inverse = lax.rsqrt(squared)
            distance = squared * inverse
            inverse_squared = inverse * inverse
            cubed = inverse * inverse_squared
            near = distance < 2.0
            scalar = jnp.where(near, 1.0 - 0.28125 * distance, 0.75 * inverse + 0.5 * cubed)
            dyadic = jnp.where(near, 0.09375 * inverse, cubed * (0.75 - 1.5 * inverse_squared))
            scaled = [dyadic * offset[c] for c in range(3)]
            for number, (a, b) in enumerate(pairs):
                value = scaled[a] * offset[b]
                if a == b:
                    value = value + scalar
                top, rest = halves(value)
                high[number, pl.ds(start, chunk), lanes] = top
                low[number, pl.ds(start, chunk), lanes] = rest
        return carry

    lax.fori_loop(0, source_count // chunk, one_chunk, 0)


def fill_columns(columns, rows):
    for c in range(3):
        for tile in range(rows.shape[1] // 128):
            lanes = slice(tile * 128, (tile + 1) * 128)
            wide = jnp.broadcast_to(rows[c : c + 1, lanes], (128, 128))
            columns[c, lanes, :] = wide.T


def apply_tiles(field, high, low):
    count = field[0].shape[0]
    parts = [halves(value) for value in field]
    both = [jnp.concatenate(part, axis=0) for part in parts]
    result = [None, None, None]

    def add(component, value):
        result[component] = value if result[component] is None else result[component] + value

    def dot(left, right):
        return jnp.dot(left, right, preferred_element_type=f32)

    for number, (a, b) in enumerate(pairs):
        if a == b:
            product = dot(both[a], high[number])
            add(a, product[:count] + product[count:])
            add(a, dot(parts[a][0], low[number]))
        else:
            product = dot(jnp.concatenate([both[a], both[b]], axis=0), high[number])
            add(b, product[:count] + product[count : 2 * count])
            add(a, product[2 * count : 3 * count] + product[3 * count :])
            product = dot(jnp.concatenate([parts[a][0], parts[b][0]], axis=0), low[number])
            add(b, product[:count])
            add(a, product[count:])
    return result


def gather_rows(pieces, rows, half):
    uppers, lowers = [], []
    start = 0
    for piece in pieces:
        for number in range(0, piece.shape[0], 2):
            upper, lower, spots = unpack_pair(piece[number], piece[number + 1], half)
            uppers.append(upper)
            lowers.append(lower)
            rows[:, start : start + spots.shape[1]] = spots
            start += spots.shape[1]
    return uppers, lowers


def side_by_side(values):
    return values[0] if len(values) == 1 else jnp.concatenate(values, axis=1)


def product_of(pieces, near_positions, scratch):
    columns, rows, high, low = scratch
    half = pieces[0].shape[1] - 8
    vectors = 2 * half // 3
    uppers, lowers = gather_rows(pieces, rows, half)
    fill_columns(columns, rows)
    build_tiles(columns, near_positions, high, low)
    field = jnp.concatenate([side_by_side(uppers), side_by_side(lowers)], axis=0)
    field = [field[c * vectors : (c + 1) * vectors] for c in range(3)]
    return jnp.concatenate(apply_tiles(field, high, low), axis=0)


def opening_part(near_positions, *refs):
    pieces, total, scratch = refs[:-5], refs[-5], refs[-4:]
    total[...] = product_of(pieces, near_positions, scratch)


def middle_part(near_positions, before, *refs):
    pieces, total, scratch = refs[:-5], refs[-5], refs[-4:]
    total[...] = before[...] + product_of(pieces, near_positions, scratch)


def closing_part(scalars, noise, near_positions, before, *refs):
    pieces, (partial, message), scratch = refs[:-6], refs[-6:-4], refs[-4:]
    width = noise.shape[1]
    value = before[...] + product_of(pieces, near_positions, scratch)
    partial[...] = value
    message[...] = value
    message[:, :width] = value[:, :width] - scalars[0:1, :width] * noise[...]


def second_kernel(scalars, nodes, near_positions, *refs):
    pieces, (high, low, weights, columns, rows) = refs[:-5], refs[-5:]
    gather_rows(pieces, rows, pieces[0].shape[1] - 8)
    fill_columns(columns, near_positions)
    build_tiles(columns, rows, high, low)
    samples = scalars[0:1, :] + scalars[4:5, :] * nodes[1:2, :]
    samples = jnp.sqrt(jnp.where(nodes[3:4, :] > 0.0, samples, 0.0))
    total = jnp.sum(samples * nodes[...], axis=1, keepdims=True)
    weights[...] = jnp.broadcast_to((2.0 / node_count) * total, weights.shape)


def swapped(value, offset, width):
    count = value.shape[1] // width
    if offset == 0:
        return value
    tiles = [value[:, 128 * t : 128 * (t + 1)] for t in range(count * width // 128)]
    per_tile = 128 // width
    inner, outer = offset % per_tile, offset // per_tile
    tiles = [tiles[t ^ outer] for t in range(len(tiles))]
    if inner:
        tiles = [pltpu.roll(tile, width, 1) for tile in tiles]
    return tiles[0] if len(tiles) == 1 else jnp.concatenate(tiles, axis=1)


def packed_block(value, number, width):
    half = value.shape[0] // 2
    block = value[:, number * width : (number + 1) * width]
    return jnp.concatenate([block[:half], block[half:]], axis=1)


def third_kernel(scalars, *refs):
    received = refs[:-9]
    partial, message, high, low, first_image, last, kept, sent, linear = refs[-9:]
    width = first_image.shape[1]
    vectors = message.shape[0] // 3
    total = message[...]
    own = partial[:, :width]
    for number, ref in enumerate(received):
        part = swapped(ref[...], number + 1, width)
        total = total + part
        own = own + part[:, :width]
    first_image[...] = own
    linear[...] = total / scalars[4:5, 0:1]
    field = [linear[c * vectors : (c + 1) * vectors, :] for c in range(3)]
    value = jnp.concatenate(apply_tiles(field, high, low), axis=0)
    count = value.shape[1] // width // 2
    for number in range(count - 1):
        kept[number] = packed_block(value, number, width)
        sent[number] = packed_block(value, count + number, width)
    last[0] = packed_block(value, count - 1, width)
    last[1] = packed_block(value, 2 * count - 1, width)


def fourth_kernel(kept, arrived, *outgoing):
    for number, ref in enumerate(outgoing):
        ref[...] = kept[number] + arrived[number]


def final_kernel(scalars, weights, noise, first_image, own, last, last_across, *refs):
    received, (displacement, images) = refs[:-2], refs[-2:]
    width = noise.shape[1]
    total = own[...] + last[0] + last_across[0]
    for ref in received:
        total = total + ref[...]
    second = jnp.concatenate([total[:, :width], total[:, width:]], axis=0)
    center = scalars[0:1, :width]
    spread = scalars[4:5, :width]
    vectors = noise[...]
    first = first_image[...]
    linear = (first - center * vectors) / spread
    quadratic = 2.0 * (second - center * linear) / spread - vectors
    displacement[...] = (
        0.5 * weights[0:1, :width] * vectors
        + weights[1:2, :width] * linear
        + weights[2:3, :width] * quadratic
    )
    images[0] = first
    images[1] = second


vmem = pl.BlockSpec(memory_space=pltpu.VMEM)


def call(kernel, inputs, outputs, scratch=(), final=False, opening=False):
    space = pltpu.HBM if opening else pltpu.VMEM
    make = jax.ShapeDtypeStruct if final else pltpu.VMEM
    sizes = [
        math.prod(ref.shape) * np.dtype(ref.dtype).itemsize
        for ref in scratch
        if ref.memory_space == pltpu.VMEM
    ]
    return pl.pallas_call(
        kernel,
        in_specs=[pl.BlockSpec(memory_space=space)] * len(inputs),
        out_shape=[make(shape, dtype) for shape, dtype in outputs],
        out_specs=[vmem] * len(outputs),
        scratch_shapes=list(scratch),
        compiler_params=pltpu.CompilerParams(vmem_limit_bytes=sum(sizes) + spare_bytes),
    )(*[pltpu.with_memory_space_constraint(value, space) for value in inputs])


def node_table():
    angles = math.pi * (np.arange(node_count) + 0.5) / node_count
    table = np.zeros((8, 128), np.float32)
    for order in range(3):
        table[order, :node_count] = np.cos(order * angles)
    table[3, :node_count] = 1.0
    return table


def combinations(masks):
    result = [0]
    for mask in masks:
        result += [value ^ mask for value in result]
    return result


def masks_for(blocks, tiles):
    bits = blocks.bit_length() - 1
    half_bits = bits // 2
    far_masks = [tiles << bit for bit in reversed(range(half_bits, bits))]
    near_masks = [1 << bit for bit in range(tiles.bit_length() - 1)]
    near_masks += [tiles << bit for bit in range(1, half_bits)]
    return tiles, far_masks, near_masks


def body(positions_in, noise_vectors, spectrum_bounds):
    core_mask, far_masks, near_masks = masks_for(lax.axis_size("blk"), lax.axis_size("tile"))
    components, vectors, width = noise_vectors.shape
    rows = components * vectors
    last = len(far_masks) - 1
    block = ((rows // 2, 2 * width), f32)

    message, noise, positions, scalars, nodes = call(
        open_kernel,
        (
            noise_vectors.reshape(rows, width),
            positions_in,
            spectrum_bounds,
            jnp.asarray(node_table()),
        ),
        [
            ((rows // 2 + 8, 2 * width), f32),
            ((rows, width), f32),
            (positions_in.shape, f32),
            ((8, 128), f32),
            ((8, 128), f32),
        ],
        (pltpu.SMEM((2,), f32), pltpu.SemaphoreType.DMA((4,))),
        opening=True,
    )
    near = positions
    far = message[None]
    near = [positions]
    near_steps = combinations(near_masks)[1:]
    for mask in near_steps:
        near.append(exchange(positions, mask))
    near = jnp.concatenate(near, axis=1)
    for mask in far_masks[:last]:
        far = jnp.concatenate([far, exchange(far, mask)], axis=0)
    across = exchange(far, core_mask)
    late = exchange(far, far_masks[last])
    late_across = exchange(late, core_mask)
    near_count, piece_count = near.shape[1], far.shape[0] * width
    far_count = 4 * piece_count

    def tiles_for(count):
        return (
            pltpu.VMEM((3, count, 128), f32),
            pltpu.VMEM((8, count), f32),
            pltpu.VMEM((6, count, near_count), bf16),
            pltpu.VMEM((6, count, near_count), bf16),
        )

    whole = ((rows, near_count), f32)
    (total,) = call(opening_part, (near, far, across), [whole], tiles_for(2 * piece_count))
    (total,) = call(middle_part, (near, total, late), [whole], tiles_for(piece_count))
    partial, message = call(
        closing_part,
        (scalars, noise, near, total, late_across),
        [whole, whole],
        tiles_for(piece_count),
    )
    high, low, weights = call(
        second_kernel,
        (scalars, nodes, near, far, late, across, late_across),
        [((6, near_count, far_count), bf16)] * 2 + [((8, 128), f32)],
        (pltpu.VMEM((3, near_count, 128), f32), pltpu.VMEM((8, far_count), f32)),
    )
    received = [exchange(message, mask) for mask in near_steps]
    far_steps = combinations(far_masks)[1:]
    several = ((len(far_steps), rows // 2, 2 * width), f32)
    first_image, last_part, kept, sent = call(
        third_kernel,
        (scalars, *received, partial, message, high, low),
        [((rows, width), f32), ((2, rows // 2, 2 * width), f32), several, several],
        (pltpu.VMEM((rows, near_count), f32),),
    )
    arrived = exchange(sent, core_mask)
    last_part = exchange(last_part, far_steps[-1])
    own, *outgoing = call(fourth_kernel, (kept, arrived), [block] * len(far_steps))
    received = [exchange(value, mask) for value, mask in zip(outgoing, far_steps)]
    last_across = exchange(last_part[1:], core_mask)
    displacement, images = call(
        final_kernel,
        (scalars, weights, noise, first_image, own, last_part, last_across, *received),
        [((rows, width), f32), ((2, rows, width), f32)],
        final=True,
    )
    shape = noise_vectors.shape
    return displacement.reshape(shape), images.reshape((2, *shape))


def solution(mesh):
    return jax.shard_map(
        body,
        mesh=mesh,
        in_specs=(P(None, axes), P(None, None, axes), P()),
        out_specs=(P(None, None, axes), P(None, None, None, axes)),
        check_vma=False,
    )
```

```python
import math

import jax
import jax.numpy as jnp
import numpy as np
from jax import lax
from jax.experimental import pallas as pl
from jax.experimental.pallas import tpu as pltpu
from jax.sharding import PartitionSpec as P

soft_core = 1e-06
node_count = 32
spare_bytes = 8 << 20
axes = ("blk", "tile")
pairs = ((0, 0), (0, 1), (0, 2), (1, 1), (1, 2), (2, 2))
f32 = jnp.float32
bf16 = jnp.bfloat16


def exchange(block, mask):
    count = lax.axis_size("blk") * lax.axis_size("tile")
    return lax.ppermute(block, axes, [(i, i ^ mask) for i in range(count)])


def open_kernel(
    noise_in, positions_in, bounds_in, nodes_in, message, noise, positions, scalars, nodes, bounds, sems
):
    moves = (
        (noise_in, noise),
        (positions_in, positions),
        (bounds_in, bounds),
        (nodes_in, nodes),
    )
    copies = [pltpu.make_async_copy(*move, sems.at[n]) for n, move in enumerate(moves)]
    for copy in copies:
        copy.start()
    for copy in copies:
        copy.wait()
    half = noise.shape[0] // 2
    message[0:half, :] = jnp.concatenate([noise[0:half, :], noise[half:, :]], axis=1)
    spot = positions[...]
    pad = jnp.zeros((8 - spot.shape[0], spot.shape[1]), f32)
    spot = jnp.concatenate([spot, pad], axis=0)
    message[half:, :] = jnp.concatenate([spot, spot], axis=1)
    highest, lowest = bounds[1], bounds[0]
    scalars[0:4, :] = jnp.full((4, 128), 0.5 * (highest + lowest), f32)
    scalars[4:8, :] = jnp.full((4, 128), 0.5 * (highest - lowest), f32)


def halves(value):
    high = value.astype(bf16)
    return high, (value - high.astype(f32)).astype(bf16)


def unpack_pair(first, second, half):
    width = first.shape[1] // 2
    left = lax.broadcasted_iota(jnp.int32, (1, 2 * width), 1) < width
    spots = jnp.where(left, first[half:], second[half:])
    first, second = first[:half], second[:half]
    upper = jnp.where(left, first, pltpu.roll(second, width, 1))
    lower = jnp.where(left, pltpu.roll(first, width, 1), second)
    return upper, lower, spots


def build_tiles(columns, target_rows, high, low):
    source_count = columns.shape[1]
    tile_count = target_rows.shape[1] // 128
    chunk = 32

    def one_chunk(step, carry):
        start = pl.multiple_of(step * chunk, chunk)
        source = [columns[c, pl.ds(start, chunk), :] for c in range(3)]
        for tile in range(tile_count):
            lanes = slice(tile * 128, (tile + 1) * 128)
            offset = [source[c] - target_rows[c : c + 1, lanes] for c in range(3)]
            squared = offset[0] * offset[0] + offset[1] * offset[1] + offset[2] * offset[2]
            squared = squared + soft_core
            inverse = lax.rsqrt(squared)
            distance = squared * inverse
            inverse_squared = inverse * inverse
            near = distance < 2.0
            scalar = jnp.where(near, 1.0 - 0.28125 * distance, inverse * (0.75 + 0.5 * inverse_squared))
            dyadic = inverse * jnp.where(near, 0.09375, inverse_squared * (0.75 - 1.5 * inverse_squared))
            scaled = [dyadic * offset[c] for c in range(3)]
            for number, (a, b) in enumerate(pairs):
                value = scaled[a] * offset[b]
                if a == b:
                    value = value + scalar
                top, rest = halves(value)
                high[number, pl.ds(start, chunk), lanes] = top
                low[number, pl.ds(start, chunk), lanes] = rest
        return carry

    lax.fori_loop(0, source_count // chunk, one_chunk, 0)


def fill_columns(columns, rows):
    for c in range(3):
        for tile in range(rows.shape[1] // 128):
            lanes = slice(tile * 128, (tile + 1) * 128)
            wide = jnp.broadcast_to(rows[c : c + 1, lanes], (128, 128))
            columns[c, lanes, :] = wide.T


def apply_tiles(field, high, low):
    count = field[0].shape[0]
    parts = [halves(value) for value in field]
    both = [jnp.concatenate(part, axis=0) for part in parts]
    result = [None, None, None]

    def add(component, value):
        result[component] = value if result[component] is None else result[component] + value

    def dot(left, right):
        return jnp.dot(left, right, preferred_element_type=f32)

    for number, (a, b) in enumerate(pairs):
        if a == b:
            product = dot(both[a], high[number])
            add(a, product[:count] + product[count:])
            add(a, dot(parts[a][0], low[number]))
        else:
            product = dot(jnp.concatenate([both[a], both[b]], axis=0), high[number])
            add(b, product[:count] + product[count : 2 * count])
            add(a, product[2 * count : 3 * count] + product[3 * count :])
            product = dot(jnp.concatenate([parts[a][0], parts[b][0]], axis=0), low[number])
            add(b, product[:count])
            add(a, product[count:])
    return result


def gather_rows(pieces, rows, half):
    uppers, lowers = [], []
    start = 0
    for piece in pieces:
        for number in range(0, piece.shape[0], 2):
            upper, lower, spots = unpack_pair(piece[number], piece[number + 1], half)
            uppers.append(upper)
            lowers.append(lower)
            rows[:, start : start + spots.shape[1]] = spots
            start += spots.shape[1]
    return uppers, lowers


def side_by_side(values):
    return values[0] if len(values) == 1 else jnp.concatenate(values, axis=1)


def product_of(pieces, near_positions, scratch):
    columns, rows, high, low = scratch
    half = pieces[0].shape[1] - 8
    vectors = 2 * half // 3
    uppers, lowers = gather_rows(pieces, rows, half)
    fill_columns(columns, rows)
    build_tiles(columns, near_positions, high, low)
    field = jnp.concatenate([side_by_side(uppers), side_by_side(lowers)], axis=0)
    field = [field[c * vectors : (c + 1) * vectors] for c in range(3)]
    return jnp.concatenate(apply_tiles(field, high, low), axis=0)


def opening_part(near_positions, *refs):
    pieces, total, scratch = refs[:-5], refs[-5], refs[-4:]
    total[...] = product_of(pieces, near_positions, scratch)


def middle_part(near_positions, before, *refs):
    pieces, total, scratch = refs[:-5], refs[-5], refs[-4:]
    total[...] = before[...] + product_of(pieces, near_positions, scratch)


def closing_part(scalars, noise, near_positions, before, *refs):
    pieces, (partial, message), scratch = refs[:-6], refs[-6:-4], refs[-4:]
    width = noise.shape[1]
    value = before[...] + product_of(pieces, near_positions, scratch)
    partial[...] = value
    message[...] = value
    message[:, :width] = value[:, :width] - scalars[0:1, :width] * noise[...]


def second_kernel(scalars, nodes, near_positions, *refs):
    pieces, (high, low, weights, columns, rows) = refs[:-5], refs[-5:]
    gather_rows(pieces, rows, pieces[0].shape[1] - 8)
    fill_columns(columns, near_positions)
    build_tiles(columns, rows, high, low)
    samples = scalars[0:1, :] + scalars[4:5, :] * nodes[1:2, :]
    samples = jnp.sqrt(jnp.where(nodes[3:4, :] > 0.0, samples, 0.0))
    total = jnp.sum(samples * nodes[...], axis=1, keepdims=True)
    weights[...] = jnp.broadcast_to((2.0 / node_count) * total, weights.shape)


def swapped(value, offset, width):
    count = value.shape[1] // width
    if offset == 0:
        return value
    tiles = [value[:, 128 * t : 128 * (t + 1)] for t in range(count * width // 128)]
    per_tile = 128 // width
    inner, outer = offset % per_tile, offset // per_tile
    tiles = [tiles[t ^ outer] for t in range(len(tiles))]
    if inner:
        tiles = [pltpu.roll(tile, width, 1) for tile in tiles]
    return tiles[0] if len(tiles) == 1 else jnp.concatenate(tiles, axis=1)


def packed_block(value, number, width):
    half = value.shape[0] // 2
    block = value[:, number * width : (number + 1) * width]
    return jnp.concatenate([block[:half], block[half:]], axis=1)


def third_kernel(scalars, *refs):
    received = refs[:-9]
    partial, message, high, low, first_image, last, kept, sent, linear = refs[-9:]
    width = first_image.shape[1]
    vectors = message.shape[0] // 3
    total = message[...]
    own = partial[:, :width]
    for number, ref in enumerate(received):
        part = swapped(ref[...], number + 1, width)
        total = total + part
        own = own + part[:, :width]
    first_image[...] = own
    linear[...] = total / scalars[4:5, 0:1]
    field = [linear[c * vectors : (c + 1) * vectors, :] for c in range(3)]
    value = jnp.concatenate(apply_tiles(field, high, low), axis=0)
    count = value.shape[1] // width // 2
    for number in range(count - 1):
        kept[number] = packed_block(value, number, width)
        sent[number] = packed_block(value, count + number, width)
    last[0] = packed_block(value, count - 1, width)
    last[1] = packed_block(value, 2 * count - 1, width)


def fourth_kernel(kept, arrived, *outgoing):
    for number, ref in enumerate(outgoing):
        ref[...] = kept[number] + arrived[number]


def final_kernel(scalars, weights, noise, first_image, own, last, last_across, *refs):
    received, (displacement, images) = refs[:-2], refs[-2:]
    width = noise.shape[1]
    total = own[...] + last[0] + last_across[0]
    for ref in received:
        total = total + ref[...]
    second = jnp.concatenate([total[:, :width], total[:, width:]], axis=0)
    center = scalars[0:1, :width]
    spread = scalars[4:5, :width]
    vectors = noise[...]
    first = first_image[...]
    linear = (first - center * vectors) / spread
    quadratic = 2.0 * (second - center * linear) / spread - vectors
    displacement[...] = (
        0.5 * weights[0:1, :width] * vectors
        + weights[1:2, :width] * linear
        + weights[2:3, :width] * quadratic
    )
    images[0] = first
    images[1] = second


vmem = pl.BlockSpec(memory_space=pltpu.VMEM)


def call(kernel, inputs, outputs, scratch=(), final=False, opening=False):
    space = pltpu.HBM if opening else pltpu.VMEM
    make = jax.ShapeDtypeStruct if final else pltpu.VMEM
    sizes = [
        math.prod(ref.shape) * np.dtype(ref.dtype).itemsize
        for ref in scratch
        if ref.memory_space == pltpu.VMEM
    ]
    return pl.pallas_call(
        kernel,
        in_specs=[pl.BlockSpec(memory_space=space)] * len(inputs),
        out_shape=[make(shape, dtype) for shape, dtype in outputs],
        out_specs=[vmem] * len(outputs),
        scratch_shapes=list(scratch),
        compiler_params=pltpu.CompilerParams(vmem_limit_bytes=sum(sizes) + spare_bytes),
    )(*[pltpu.with_memory_space_constraint(value, space) for value in inputs])


def node_table():
    angles = math.pi * (np.arange(node_count) + 0.5) / node_count
    table = np.zeros((8, 128), np.float32)
    for order in range(3):
        table[order, :node_count] = np.cos(order * angles)
    table[3, :node_count] = 1.0
    return table


def combinations(masks):
    result = [0]
    for mask in masks:
        result += [value ^ mask for value in result]
    return result


def masks_for(blocks, tiles):
    bits = blocks.bit_length() - 1
    half_bits = bits // 2
    far_masks = [tiles << bit for bit in reversed(range(half_bits, bits))]
    near_masks = [1 << bit for bit in range(tiles.bit_length() - 1)]
    near_masks += [tiles << bit for bit in range(1, half_bits)]
    return tiles, [mask ^ tiles for mask in far_masks], [mask ^ tiles for mask in near_masks]


def body(positions_in, noise_vectors, spectrum_bounds):
    core_mask, far_masks, near_masks = masks_for(lax.axis_size("blk"), lax.axis_size("tile"))
    components, vectors, width = noise_vectors.shape
    rows = components * vectors
    last = len(far_masks) - 1
    block = ((rows // 2, 2 * width), f32)

    message, noise, positions, scalars, nodes = call(
        open_kernel,
        (
            noise_vectors.reshape(rows, width),
            positions_in,
            spectrum_bounds,
            jnp.asarray(node_table()),
        ),
        [
            ((rows // 2 + 8, 2 * width), f32),
            ((rows, width), f32),
            (positions_in.shape, f32),
            ((8, 128), f32),
            ((8, 128), f32),
        ],
        (pltpu.SMEM((2,), f32), pltpu.SemaphoreType.DMA((4,))),
        opening=True,
    )
    near = positions
    far = message[None]
    near = [positions]
    near_steps = combinations(near_masks)[1:]
    for mask in near_steps:
        near.append(exchange(positions, mask))
    near = jnp.concatenate(near, axis=1)
    for mask in far_masks[:last]:
        far = jnp.concatenate([far, exchange(far, mask)], axis=0)
    across = exchange(far, core_mask)
    late = exchange(far, far_masks[last])
    late_across = exchange(late, core_mask)
    near_count, piece_count = near.shape[1], far.shape[0] * width
    far_count = 4 * piece_count

    def tiles_for(count):
        return (
            pltpu.VMEM((3, count, 128), f32),
            pltpu.VMEM((8, count), f32),
            pltpu.VMEM((6, count, near_count), bf16),
            pltpu.VMEM((6, count, near_count), bf16),
        )

    whole = ((rows, near_count), f32)
    (total,) = call(opening_part, (near, far, across), [whole], tiles_for(2 * piece_count))
    (total,) = call(middle_part, (near, total, late), [whole], tiles_for(piece_count))
    partial, message = call(
        closing_part,
        (scalars, noise, near, total, late_across),
        [whole, whole],
        tiles_for(piece_count),
    )
    high, low, weights = call(
        second_kernel,
        (scalars, nodes, near, far, late, across, late_across),
        [((6, near_count, far_count), bf16)] * 2 + [((8, 128), f32)],
        (pltpu.VMEM((3, near_count, 128), f32), pltpu.VMEM((8, far_count), f32)),
    )
    received = [exchange(message, mask) for mask in near_steps]
    far_steps = combinations(far_masks)[1:]
    several = ((len(far_steps), rows // 2, 2 * width), f32)
    first_image, last_part, kept, sent = call(
        third_kernel,
        (scalars, *received, partial, message, high, low),
        [((rows, width), f32), ((2, rows // 2, 2 * width), f32), several, several],
        (pltpu.VMEM((rows, near_count), f32),),
    )
    arrived = exchange(sent, core_mask)
    last_part = exchange(last_part, far_steps[-1])
    own, *outgoing = call(fourth_kernel, (kept, arrived), [block] * len(far_steps))
    received = [exchange(value, mask) for value, mask in zip(outgoing, far_steps)]
    last_across = exchange(last_part[1:], core_mask)
    displacement, images = call(
        final_kernel,
        (scalars, weights, noise, first_image, own, last_part, last_across, *received),
        [((rows, width), f32), ((2, rows, width), f32)],
        final=True,
    )
    shape = noise_vectors.shape
    return displacement.reshape(shape), images.reshape((2, *shape))


def solution(mesh):
    return jax.shard_map(
        body,
        mesh=mesh,
        in_specs=(P(None, axes), P(None, None, axes), P()),
        out_specs=(P(None, None, axes), P(None, None, None, axes)),
        check_vma=False,
    )
```

```python
import functools
import math

import jax
import jax.numpy as jnp
import numpy as np
from jax import lax
from jax.experimental import pallas as pl
from jax.experimental.pallas import tpu as pltpu
from jax.sharding import PartitionSpec as P

soft_core = 1e-06
node_count = 32
spare_bytes = 8 << 20
axes = ("blk", "tile")
pairs = ((0, 0), (0, 1), (0, 2), (1, 1), (1, 2), (2, 2))
f32 = jnp.float32
bf16 = jnp.bfloat16


def exchange(block, mask):
    count = lax.axis_size("blk") * lax.axis_size("tile")
    return lax.ppermute(block, axes, [(i, i ^ mask) for i in range(count)])


def open_kernel(
    noise_in, positions_in, bounds_in, nodes_in, message, noise, positions, scalars, nodes, bounds, sems
):
    moves = (
        (noise_in, noise),
        (positions_in, positions),
        (bounds_in, bounds),
        (nodes_in, nodes),
    )
    copies = [pltpu.make_async_copy(*move, sems.at[n]) for n, move in enumerate(moves)]
    for copy in copies:
        copy.start()
    copies[0].wait()
    copies[1].wait()
    half = noise.shape[0] // 2
    message[0:half, :] = jnp.concatenate([noise[0:half, :], noise[half:, :]], axis=1)
    spot = positions[...]
    pad = jnp.zeros((8 - spot.shape[0], spot.shape[1]), f32)
    spot = jnp.concatenate([spot, pad], axis=0)
    message[half:, :] = jnp.concatenate([spot, spot], axis=1)
    copies[2].wait()
    copies[3].wait()
    highest, lowest = bounds[1], bounds[0]
    scalars[0:4, :] = jnp.full((4, 128), 0.5 * (highest + lowest), f32)
    scalars[4:8, :] = jnp.full((4, 128), 0.5 * (highest - lowest), f32)


def halves(value):
    high = value.astype(bf16)
    return high, (value - high.astype(f32)).astype(bf16)


def unpack_pair(first, second, half):
    width = first.shape[1] // 2
    left = lax.broadcasted_iota(jnp.int32, (1, 2 * width), 1) < width
    spots = jnp.where(left, first[half:], second[half:])
    first, second = first[:half], second[:half]
    upper = jnp.where(left, first, pltpu.roll(second, width, 1))
    lower = jnp.where(left, pltpu.roll(first, width, 1), second)
    return upper, lower, spots


def build_tiles(columns, target_rows, high, low):
    source_count = columns.shape[1]
    tile_count = target_rows.shape[1] // 128
    chunk = 64

    def one_chunk(step, carry):
        start = pl.multiple_of(step * chunk, chunk)
        source = [columns[c, pl.ds(start, chunk), :] for c in range(3)]
        for tile in range(tile_count):
            lanes = slice(tile * 128, (tile + 1) * 128)
            offset = [source[c] - target_rows[c : c + 1, lanes] for c in range(3)]
            squared = offset[0] * offset[0] + offset[1] * offset[1] + offset[2] * offset[2]
            squared = squared + soft_core
            inverse = lax.rsqrt(squared)
            distance = squared * inverse
            inverse_squared = inverse * inverse
            near = distance < 2.0
            scalar = jnp.where(near, 1.0 - 0.28125 * distance, inverse * (0.75 + 0.5 * inverse_squared))
            dyadic = inverse * jnp.where(near, 0.09375, inverse_squared * (0.75 - 1.5 * inverse_squared))
            scaled = [dyadic * offset[c] for c in range(3)]
            for number, (a, b) in enumerate(pairs):
                value = scaled[a] * offset[b]
                if a == b:
                    value = value + scalar
                top, rest = halves(value)
                high[number, pl.ds(start, chunk), lanes] = top
                low[number, pl.ds(start, chunk), lanes] = rest
        return carry

    lax.fori_loop(0, source_count // chunk, one_chunk, 0)


def fill_columns(columns, rows):
    for c in range(3):
        for tile in range(rows.shape[1] // 128):
            lanes = slice(tile * 128, (tile + 1) * 128)
            wide = jnp.broadcast_to(rows[c : c + 1, lanes], (128, 128))
            columns[c, lanes, :] = wide.T


def apply_tiles(field, high, low):
    count = field[0].shape[0]
    parts = [halves(value) for value in field]
    both = [jnp.concatenate(part, axis=0) for part in parts]
    result = [None, None, None]

    def add(component, value):
        result[component] = value if result[component] is None else result[component] + value

    def dot(left, right):
        return jnp.dot(left, right, preferred_element_type=f32)

    for number, (a, b) in enumerate(pairs):
        if a == b:
            product = dot(both[a], high[number])
            add(a, product[:count] + product[count:])
            add(a, dot(parts[a][0], low[number]))
        else:
            product = dot(jnp.concatenate([both[a], both[b]], axis=0), high[number])
            add(b, product[:count] + product[count : 2 * count])
            add(a, product[2 * count : 3 * count] + product[3 * count :])
            product = dot(jnp.concatenate([parts[a][0], parts[b][0]], axis=0), low[number])
            add(b, product[:count])
            add(a, product[count:])
    return result


def gather_rows(pieces, rows, half):
    uppers, lowers = [], []
    start = 0
    for piece in pieces:
        for number in range(0, piece.shape[0], 2):
            upper, lower, spots = unpack_pair(piece[number], piece[number + 1], half)
            uppers.append(upper)
            lowers.append(lower)
            rows[:, start : start + spots.shape[1]] = spots
            start += spots.shape[1]
    return uppers, lowers


def side_by_side(values):
    return values[0] if len(values) == 1 else jnp.concatenate(values, axis=1)


def product_of(pieces, near_positions, scratch):
    columns, rows, high, low = scratch
    half = pieces[0].shape[1] - 8
    vectors = 2 * half // 3
    uppers, lowers = gather_rows(pieces, rows, half)
    fill_columns(columns, rows)
    build_tiles(columns, near_positions, high, low)
    field = jnp.concatenate([side_by_side(uppers), side_by_side(lowers)], axis=0)
    field = [field[c * vectors : (c + 1) * vectors] for c in range(3)]
    return jnp.concatenate(apply_tiles(field, high, low), axis=0)


def opening_part(near_positions, *refs):
    pieces, total, scratch = refs[:-5], refs[-5], refs[-4:]
    total[...] = product_of(pieces, near_positions, scratch)


def middle_part(near_positions, before, *refs):
    pieces, total, scratch = refs[:-5], refs[-5], refs[-4:]
    total[...] = before[...] + product_of(pieces, near_positions, scratch)


def closing_part(scalars, noise, near_positions, before, *refs):
    pieces, (partial, message), scratch = refs[:-6], refs[-6:-4], refs[-4:]
    width = noise.shape[1]
    value = before[...] + product_of(pieces, near_positions, scratch)
    partial[...] = value
    message[...] = value
    message[:, :width] = value[:, :width] - scalars[0:1, :width] * noise[...]


def second_kernel(scalars, nodes, near_positions, *refs):
    pieces, (high, low, weights, columns, rows) = refs[:-5], refs[-5:]
    gather_rows(pieces, rows, pieces[0].shape[1] - 8)
    fill_columns(columns, near_positions)
    build_tiles(columns, rows, high, low)
    samples = scalars[0:1, :] + scalars[4:5, :] * nodes[1:2, :]
    samples = jnp.sqrt(jnp.where(nodes[3:4, :] > 0.0, samples, 0.0))
    total = jnp.sum(samples * nodes[...], axis=1, keepdims=True)
    weights[...] = jnp.broadcast_to((2.0 / node_count) * total, weights.shape)


def swapped(value, offset, width):
    count = value.shape[1] // width
    if offset == 0:
        return value
    tiles = [value[:, 128 * t : 128 * (t + 1)] for t in range(count * width // 128)]
    per_tile = 128 // width
    inner, outer = offset % per_tile, offset // per_tile
    tiles = [tiles[t ^ outer] for t in range(len(tiles))]
    if inner:
        tiles = [pltpu.roll(tile, width, 1) for tile in tiles]
    return tiles[0] if len(tiles) == 1 else jnp.concatenate(tiles, axis=1)


def packed_block(value, number, width):
    half = value.shape[0] // 2
    block = value[:, number * width : (number + 1) * width]
    return jnp.concatenate([block[:half], block[half:]], axis=1)


def third_kernel(scalars, *refs):
    received = refs[:-9]
    partial, message, high, low, first_image, last, kept, sent, linear = refs[-9:]
    width = first_image.shape[1]
    vectors = message.shape[0] // 3
    total = message[...]
    own = partial[:, :width]
    for number, ref in enumerate(received):
        part = swapped(ref[...], number + 1, width)
        total = total + part
        own = own + part[:, :width]
    first_image[...] = own
    linear[...] = total / scalars[4:5, 0:1]
    field = [linear[c * vectors : (c + 1) * vectors, :] for c in range(3)]
    value = jnp.concatenate(apply_tiles(field, high, low), axis=0)
    count = value.shape[1] // width // 2
    for number in range(count - 1):
        kept[number] = packed_block(value, number, width)
        sent[number] = packed_block(value, count + number, width)
    last[0] = packed_block(value, count - 1, width)
    last[1] = packed_block(value, 2 * count - 1, width)


def fourth_kernel(kept, arrived, *outgoing):
    for number, ref in enumerate(outgoing):
        ref[...] = kept[number] + arrived[number]


def final_kernel(mine, scalars, weights, noise, first_image, own, last, last_across, *refs):
    received, (displacement, images) = refs[:-2], refs[-2:]
    width = noise.shape[1]
    total = own[...] + last[mine] + last_across[1 - mine]
    for ref in received:
        total = total + ref[...]
    second = jnp.concatenate([total[:, :width], total[:, width:]], axis=0)
    center = scalars[0:1, :width]
    spread = scalars[4:5, :width]
    vectors = noise[...]
    first = first_image[...]
    linear = (first - center * vectors) / spread
    quadratic = 2.0 * (second - center * linear) / spread - vectors
    displacement[...] = (
        0.5 * weights[0:1, :width] * vectors
        + weights[1:2, :width] * linear
        + weights[2:3, :width] * quadratic
    )
    images[0] = first
    images[1] = second


vmem = pl.BlockSpec(memory_space=pltpu.VMEM)


def call(kernel, inputs, outputs, scratch=(), final=False, opening=False):
    space = pltpu.HBM if opening else pltpu.VMEM
    make = jax.ShapeDtypeStruct if final else pltpu.VMEM
    sizes = [
        math.prod(ref.shape) * np.dtype(ref.dtype).itemsize
        for ref in scratch
        if ref.memory_space == pltpu.VMEM
    ]
    return pl.pallas_call(
        kernel,
        in_specs=[pl.BlockSpec(memory_space=space)] * len(inputs),
        out_shape=[make(shape, dtype) for shape, dtype in outputs],
        out_specs=[vmem] * len(outputs),
        scratch_shapes=list(scratch),
        compiler_params=pltpu.CompilerParams(vmem_limit_bytes=sum(sizes) + spare_bytes),
    )(*[pltpu.with_memory_space_constraint(value, space) for value in inputs])


def node_table():
    angles = math.pi * (np.arange(node_count) + 0.5) / node_count
    table = np.zeros((8, 128), np.float32)
    for order in range(3):
        table[order, :node_count] = np.cos(order * angles)
    table[3, :node_count] = 1.0
    return table


def combinations(masks):
    result = [0]
    for mask in masks:
        result += [value ^ mask for value in result]
    return result


def masks_for(blocks, tiles):
    bits = blocks.bit_length() - 1
    half_bits = bits // 2
    far_masks = [tiles << bit for bit in reversed(range(half_bits, bits))]
    near_masks = [1 << bit for bit in range(tiles.bit_length() - 1)]
    near_masks += [tiles << bit for bit in range(1, half_bits)]
    return tiles, [mask ^ tiles for mask in far_masks], [mask ^ tiles for mask in near_masks]


def body(positions_in, noise_vectors, spectrum_bounds):
    core_mask, far_masks, near_masks = masks_for(lax.axis_size("blk"), lax.axis_size("tile"))
    components, vectors, width = noise_vectors.shape
    rows = components * vectors
    last = len(far_masks) - 1
    block = ((rows // 2, 2 * width), f32)

    message, noise, positions, scalars, nodes = call(
        open_kernel,
        (
            noise_vectors.reshape(rows, width),
            positions_in,
            spectrum_bounds,
            jnp.asarray(node_table()),
        ),
        [
            ((rows // 2 + 8, 2 * width), f32),
            ((rows, width), f32),
            (positions_in.shape, f32),
            ((8, 128), f32),
            ((8, 128), f32),
        ],
        (pltpu.SMEM((2,), f32), pltpu.SemaphoreType.DMA((4,))),
        opening=True,
    )
    near = positions
    far = message[None]
    near = [positions]
    near_steps = combinations(near_masks)[1:]
    for mask in near_steps:
        near.append(exchange(positions, mask))
    near = jnp.concatenate(near, axis=1)
    for mask in far_masks[:last]:
        far = jnp.concatenate([far, exchange(far, mask)], axis=0)
    across = exchange(far, core_mask)
    late = exchange(far, far_masks[last])
    late_across = exchange(late, core_mask)
    near_count, piece_count = near.shape[1], far.shape[0] * width
    far_count = 4 * piece_count

    def tiles_for(count):
        return (
            pltpu.VMEM((3, count, 128), f32),
            pltpu.VMEM((8, count), f32),
            pltpu.VMEM((6, count, near_count), bf16),
            pltpu.VMEM((6, count, near_count), bf16),
        )

    whole = ((rows, near_count), f32)
    (total,) = call(opening_part, (near, far, across), [whole], tiles_for(2 * piece_count))
    (total,) = call(middle_part, (near, total, late), [whole], tiles_for(piece_count))
    partial, message = call(
        closing_part,
        (scalars, noise, near, total, late_across),
        [whole, whole],
        tiles_for(piece_count),
    )
    high, low, weights = call(
        second_kernel,
        (scalars, nodes, near, far, late, across, late_across),
        [((6, near_count, far_count), bf16)] * 2 + [((8, 128), f32)],
        (pltpu.VMEM((3, near_count, 128), f32), pltpu.VMEM((8, far_count), f32)),
    )
    received = [exchange(message, mask) for mask in near_steps]
    far_steps = combinations(far_masks)[1:]
    several = ((len(far_steps), rows // 2, 2 * width), f32)
    first_image, last_part, kept, sent = call(
        third_kernel,
        (scalars, *received, partial, message, high, low),
        [((rows, width), f32), ((2, rows // 2, 2 * width), f32), several, several],
        (pltpu.VMEM((rows, near_count), f32),),
    )
    arrived = exchange(sent, core_mask)
    straight = int(far_steps[-1] & core_mask == 0)
    last_part = exchange(last_part, far_steps[-1] ^ straight * core_mask)
    own, *outgoing = call(fourth_kernel, (kept, arrived), [block] * len(far_steps))
    received = [exchange(value, mask) for value, mask in zip(outgoing, far_steps)]
    last_across = exchange(last_part, core_mask)
    displacement, images = call(
        functools.partial(final_kernel, straight),
        (scalars, weights, noise, first_image, own, last_part, last_across, *received),
        [((rows, width), f32), ((2, rows, width), f32)],
        final=True,
    )
    shape = noise_vectors.shape
    return displacement.reshape(shape), images.reshape((2, *shape))


def solution(mesh):
    return jax.shard_map(
        body,
        mesh=mesh,
        in_specs=(P(None, axes), P(None, None, axes), P()),
        out_specs=(P(None, None, axes), P(None, None, None, axes)),
        check_vma=False,
    )
```

```python
import functools
import math

import jax
import jax.numpy as jnp
import numpy as np
from jax import lax
from jax.experimental import pallas as pl
from jax.experimental.pallas import tpu as pltpu
from jax.sharding import PartitionSpec as P

soft_core = 1e-06
node_count = 32
spare_bytes = 8 << 20
axes = ("blk", "tile")
pairs = ((0, 0), (0, 1), (0, 2), (1, 1), (1, 2), (2, 2))
f32 = jnp.float32
bf16 = jnp.bfloat16


def exchange(block, mask):
    count = lax.axis_size("blk") * lax.axis_size("tile")
    return lax.ppermute(block, axes, [(i, i ^ mask) for i in range(count)])


def open_kernel(
    noise_in, positions_in, bounds_in, nodes_in, message, noise, positions, scalars, nodes, bounds, sems
):
    moves = (
        (noise_in, noise),
        (positions_in, positions),
        (bounds_in, bounds),
        (nodes_in, nodes),
    )
    copies = [pltpu.make_async_copy(*move, sems.at[n]) for n, move in enumerate(moves)]
    for copy in copies:
        copy.start()
    for copy in copies:
        copy.wait()
    half = noise.shape[0] // 2
    message[0:half, :] = jnp.concatenate([noise[0:half, :], noise[half:, :]], axis=1)
    spot = positions[...]
    pad = jnp.zeros((8 - spot.shape[0], spot.shape[1]), f32)
    spot = jnp.concatenate([spot, pad], axis=0)
    message[half:, :] = jnp.concatenate([spot, spot], axis=1)
    highest, lowest = bounds[1], bounds[0]
    scalars[0:4, :] = jnp.full((4, 128), 0.5 * (highest + lowest), f32)
    scalars[4:8, :] = jnp.full((4, 128), 0.5 * (highest - lowest), f32)


def halves(value):
    high = value.astype(bf16)
    return high, (value - high.astype(f32)).astype(bf16)


def unpack_pair(first, second, half):
    width = first.shape[1] // 2
    left = lax.broadcasted_iota(jnp.int32, (1, 2 * width), 1) < width
    spots = jnp.where(left, first[half:], second[half:])
    first, second = first[:half], second[:half]
    upper = jnp.where(left, first, pltpu.roll(second, width, 1))
    lower = jnp.where(left, pltpu.roll(first, width, 1), second)
    return upper, lower, spots


def build_tiles(columns, target_rows, high, low):
    source_count = columns.shape[1]
    tile_count = target_rows.shape[1] // 128
    chunk = 64

    def one_chunk(step, carry):
        start = pl.multiple_of(step * chunk, chunk)
        source = [columns[c, pl.ds(start, chunk), :] for c in range(3)]
        for tile in range(tile_count):
            lanes = slice(tile * 128, (tile + 1) * 128)
            offset = [source[c] - target_rows[c : c + 1, lanes] for c in range(3)]
            squared = offset[0] * offset[0] + offset[1] * offset[1] + offset[2] * offset[2]
            squared = squared + soft_core
            inverse = lax.rsqrt(squared)
            distance = squared * inverse
            inverse_squared = inverse * inverse
            near = distance < 2.0
            scalar = jnp.where(near, 1.0 - 0.28125 * distance, inverse * (0.75 + 0.5 * inverse_squared))
            dyadic = inverse * jnp.where(near, 0.09375, inverse_squared * (0.75 - 1.5 * inverse_squared))
            scaled = [dyadic * offset[c] for c in range(3)]
            for number, (a, b) in enumerate(pairs):
                value = scaled[a] * offset[b]
                if a == b:
                    value = value + scalar
                top, rest = halves(value)
                high[number, pl.ds(start, chunk), lanes] = top
                low[number, pl.ds(start, chunk), lanes] = rest
        return carry

    lax.fori_loop(0, source_count // chunk, one_chunk, 0)


def fill_columns(columns, rows):
    for c in range(3):
        for tile in range(rows.shape[1] // 128):
            lanes = slice(tile * 128, (tile + 1) * 128)
            wide = jnp.broadcast_to(rows[c : c + 1, lanes], (128, 128))
            columns[c, lanes, :] = wide.T


def apply_tiles(field, high, low):
    count = field[0].shape[0]
    parts = [halves(value) for value in field]
    both = [jnp.concatenate(part, axis=0) for part in parts]
    result = [None, None, None]

    def add(component, value):
        result[component] = value if result[component] is None else result[component] + value

    def dot(left, right):
        return jnp.dot(left, right, preferred_element_type=f32)

    for number, (a, b) in enumerate(pairs):
        if a == b:
            product = dot(both[a], high[number])
            add(a, product[:count] + product[count:])
            add(a, dot(parts[a][0], low[number]))
        else:
            product = dot(jnp.concatenate([both[a], both[b]], axis=0), high[number])
            add(b, product[:count] + product[count : 2 * count])
            add(a, product[2 * count : 3 * count] + product[3 * count :])
            product = dot(jnp.concatenate([parts[a][0], parts[b][0]], axis=0), low[number])
            add(b, product[:count])
            add(a, product[count:])
    return result


def gather_rows(pieces, rows, half):
    uppers, lowers = [], []
    start = 0
    for piece in pieces:
        for number in range(0, piece.shape[0], 2):
            upper, lower, spots = unpack_pair(piece[number], piece[number + 1], half)
            uppers.append(upper)
            lowers.append(lower)
            rows[:, start : start + spots.shape[1]] = spots
            start += spots.shape[1]
    return uppers, lowers


def side_by_side(values):
    return values[0] if len(values) == 1 else jnp.concatenate(values, axis=1)


def product_of(pieces, near_positions, scratch):
    columns, rows, high, low = scratch
    half = pieces[0].shape[1] - 8
    vectors = 2 * half // 3
    uppers, lowers = gather_rows(pieces, rows, half)
    fill_columns(columns, rows)
    build_tiles(columns, near_positions, high, low)
    field = jnp.concatenate([side_by_side(uppers), side_by_side(lowers)], axis=0)
    field = [field[c * vectors : (c + 1) * vectors] for c in range(3)]
    return jnp.concatenate(apply_tiles(field, high, low), axis=0)


def opening_part(near_positions, *refs):
    pieces, total, scratch = refs[:-5], refs[-5], refs[-4:]
    total[...] = product_of(pieces, near_positions, scratch)


def middle_part(near_positions, before, *refs):
    pieces, total, scratch = refs[:-5], refs[-5], refs[-4:]
    total[...] = before[...] + product_of(pieces, near_positions, scratch)


def closing_part(scalars, noise, near_positions, before, *refs):
    pieces, (partial, message), scratch = refs[:-6], refs[-6:-4], refs[-4:]
    width = noise.shape[1]
    value = before[...] + product_of(pieces, near_positions, scratch)
    partial[...] = value
    message[...] = value
    message[:, :width] = value[:, :width] - scalars[0:1, :width] * noise[...]


def second_kernel(scalars, nodes, near_positions, *refs):
    pieces, (high, low, weights, columns, rows) = refs[:-5], refs[-5:]
    gather_rows(pieces, rows, pieces[0].shape[1] - 8)
    fill_columns(columns, near_positions)
    build_tiles(columns, rows, high, low)
    samples = scalars[0:1, :] + scalars[4:5, :] * nodes[1:2, :]
    samples = jnp.sqrt(jnp.where(nodes[3:4, :] > 0.0, samples, 0.0))
    total = jnp.sum(samples * nodes[...], axis=1, keepdims=True)
    weights[...] = jnp.broadcast_to((2.0 / node_count) * total, weights.shape)


def swapped(value, offset, width):
    count = value.shape[1] // width
    if offset == 0:
        return value
    tiles = [value[:, 128 * t : 128 * (t + 1)] for t in range(count * width // 128)]
    per_tile = 128 // width
    inner, outer = offset % per_tile, offset // per_tile
    tiles = [tiles[t ^ outer] for t in range(len(tiles))]
    if inner:
        tiles = [pltpu.roll(tile, width, 1) for tile in tiles]
    return tiles[0] if len(tiles) == 1 else jnp.concatenate(tiles, axis=1)


def packed_block(value, number, width):
    half = value.shape[0] // 2
    block = value[:, number * width : (number + 1) * width]
    return jnp.concatenate([block[:half], block[half:]], axis=1)


def third_kernel(scalars, *refs):
    received = refs[:-9]
    partial, message, high, low, first_image, last, kept, sent, linear = refs[-9:]
    width = first_image.shape[1]
    vectors = message.shape[0] // 3
    total = message[...]
    own = partial[:, :width]
    for number, ref in enumerate(received):
        part = swapped(ref[...], number + 1, width)
        total = total + part
        own = own + part[:, :width]
    linear[...] = total / scalars[4:5, 0:1]
    field = [linear[c * vectors : (c + 1) * vectors, :] for c in range(3)]
    value = jnp.concatenate(apply_tiles(field, high, low), axis=0)
    count = value.shape[1] // width // 2
    for number in range(count - 1):
        kept[number] = packed_block(value, number, width)
        sent[number] = packed_block(value, count + number, width)
    last[0] = packed_block(value, count - 1, width)
    last[1] = packed_block(value, 2 * count - 1, width)
    first_image[...] = own


def fourth_kernel(kept, arrived, *outgoing):
    for number, ref in enumerate(outgoing):
        ref[...] = kept[number] + arrived[number]


def final_kernel(mine, scalars, weights, noise, first_image, own, last, last_across, *refs):
    received, (displacement, images) = refs[:-2], refs[-2:]
    width = noise.shape[1]
    total = own[...] + last[mine] + last_across[1 - mine]
    for ref in received:
        total = total + ref[...]
    second = jnp.concatenate([total[:, :width], total[:, width:]], axis=0)
    center = scalars[0:1, :width]
    spread = scalars[4:5, :width]
    vectors = noise[...]
    first = first_image[...]
    linear = (first - center * vectors) / spread
    quadratic = 2.0 * (second - center * linear) / spread - vectors
    displacement[...] = (
        0.5 * weights[0:1, :width] * vectors
        + weights[1:2, :width] * linear
        + weights[2:3, :width] * quadratic
    )
    images[0] = first
    images[1] = second


vmem = pl.BlockSpec(memory_space=pltpu.VMEM)


def call(kernel, inputs, outputs, scratch=(), final=False, opening=False):
    space = pltpu.HBM if opening else pltpu.VMEM
    make = jax.ShapeDtypeStruct if final else pltpu.VMEM
    sizes = [
        math.prod(ref.shape) * np.dtype(ref.dtype).itemsize
        for ref in scratch
        if ref.memory_space == pltpu.VMEM
    ]
    return pl.pallas_call(
        kernel,
        in_specs=[pl.BlockSpec(memory_space=space)] * len(inputs),
        out_shape=[make(shape, dtype) for shape, dtype in outputs],
        out_specs=[vmem] * len(outputs),
        scratch_shapes=list(scratch),
        compiler_params=pltpu.CompilerParams(vmem_limit_bytes=sum(sizes) + spare_bytes),
    )(*[pltpu.with_memory_space_constraint(value, space) for value in inputs])


def node_table():
    angles = math.pi * (np.arange(node_count) + 0.5) / node_count
    table = np.zeros((8, 128), np.float32)
    for order in range(3):
        table[order, :node_count] = np.cos(order * angles)
    table[3, :node_count] = 1.0
    return table


def combinations(masks):
    result = [0]
    for mask in masks:
        result += [value ^ mask for value in result]
    return result


def masks_for(blocks, tiles):
    bits = blocks.bit_length() - 1
    half_bits = bits // 2
    far_masks = [tiles << bit for bit in reversed(range(half_bits, bits))]
    near_masks = [1 << bit for bit in range(tiles.bit_length() - 1)]
    near_masks += [tiles << bit for bit in range(1, half_bits)]
    return tiles, [mask ^ tiles for mask in far_masks], [mask ^ tiles for mask in near_masks]


def body(positions_in, noise_vectors, spectrum_bounds):
    core_mask, far_masks, near_masks = masks_for(lax.axis_size("blk"), lax.axis_size("tile"))
    components, vectors, width = noise_vectors.shape
    rows = components * vectors
    last = len(far_masks) - 1
    block = ((rows // 2, 2 * width), f32)

    message, noise, positions, scalars, nodes = call(
        open_kernel,
        (
            noise_vectors.reshape(rows, width),
            positions_in,
            spectrum_bounds,
            jnp.asarray(node_table()),
        ),
        [
            ((rows // 2 + 8, 2 * width), f32),
            ((rows, width), f32),
            (positions_in.shape, f32),
            ((8, 128), f32),
            ((8, 128), f32),
        ],
        (pltpu.SMEM((2,), f32), pltpu.SemaphoreType.DMA((4,))),
        opening=True,
    )
    near = positions
    far = message[None]
    near = [positions]
    near_steps = combinations(near_masks)[1:]
    for mask in near_steps:
        near.append(exchange(positions, mask))
    near = jnp.concatenate(near, axis=1)
    for mask in far_masks[:last]:
        far = jnp.concatenate([far, exchange(far, mask)], axis=0)
    across = exchange(far, core_mask)
    late = exchange(far, far_masks[last])
    late_across = exchange(late, core_mask)
    near_count, piece_count = near.shape[1], far.shape[0] * width
    far_count = 4 * piece_count

    def tiles_for(count):
        return (
            pltpu.VMEM((3, count, 128), f32),
            pltpu.VMEM((8, count), f32),
            pltpu.VMEM((6, count, near_count), bf16),
            pltpu.VMEM((6, count, near_count), bf16),
        )

    whole = ((rows, near_count), f32)
    (total,) = call(opening_part, (near, far, across), [whole], tiles_for(2 * piece_count))
    (total,) = call(middle_part, (near, total, late), [whole], tiles_for(piece_count))
    partial, message = call(
        closing_part,
        (scalars, noise, near, total, late_across),
        [whole, whole],
        tiles_for(piece_count),
    )
    high, low, weights = call(
        second_kernel,
        (scalars, nodes, near, far, late, across, late_across),
        [((6, near_count, far_count), bf16)] * 2 + [((8, 128), f32)],
        (pltpu.VMEM((3, near_count, 128), f32), pltpu.VMEM((8, far_count), f32)),
    )
    received = [exchange(message, mask) for mask in near_steps]
    far_steps = combinations(far_masks)[1:]
    several = ((len(far_steps), rows // 2, 2 * width), f32)
    first_image, last_part, kept, sent = call(
        third_kernel,
        (scalars, *received, partial, message, high, low),
        [((rows, width), f32), ((2, rows // 2, 2 * width), f32), several, several],
        (pltpu.VMEM((rows, near_count), f32),),
    )
    arrived = exchange(sent, core_mask)
    straight = int(far_steps[-1] & core_mask == 0)
    last_part = exchange(last_part, far_steps[-1] ^ straight * core_mask)
    own, *outgoing = call(fourth_kernel, (kept, arrived), [block] * len(far_steps))
    received = [exchange(value, mask) for value, mask in zip(outgoing, far_steps)]
    last_across = exchange(last_part, core_mask)
    displacement, images = call(
        functools.partial(final_kernel, straight),
        (scalars, weights, noise, first_image, own, last_part, last_across, *received),
        [((rows, width), f32), ((2, rows, width), f32)],
        final=True,
    )
    shape = noise_vectors.shape
    return displacement.reshape(shape), images.reshape((2, *shape))


def solution(mesh):
    return jax.shard_map(
        body,
        mesh=mesh,
        in_specs=(P(None, axes), P(None, None, axes), P()),
        out_specs=(P(None, None, axes), P(None, None, None, axes)),
        check_vma=False,
    )
```
